128 devices in a mesh: seq: 16 (over y, z), grp: 8 (over x, core).
Axes of the slice: x: 4, y: 4, z: 4, core: 2. Of those that a mesh axis runs over, the one named last changes fastest.
Arguments:
- queries: bfloat16 [16384, 1024], P(('grp', 'seq')), may hold values from -160 to 160
- states: bfloat16 [16384, 1024], P(('grp', 'seq')), may hold values from -6 to 6
- behavior_keys: bfloat16 [16, 4096, 1024], P('grp', 'seq'), may hold values from -7 to 7
- behavior_values: bfloat16 [16, 4096, 1024], P('grp', 'seq'), may hold values from -6 to 6
- lengths: int32 [16], P('grp'), may hold values from 1024 to 4096, as said below
- user_of: int32 [16384], P('grp'), may hold values from 0 to 1
- out_weight: bfloat16 [1024, 1024], replicated, may hold values from -0.1875 to 0.1875
- norm_gain: float32 [1024], replicated, may hold values from 0.1 to 1.9
- routes: int32 [16384, 2], P(('grp', 'seq')), may hold values from 0 to 127, all different within a row; in each aligned block of 256 rows (0 to 255, 256 to 511, ...) at most 4 rows name the same one
- route_weights: float32 [16384, 2], P(('grp', 'seq')), may hold values from 0.25 to 1
- expert_up: bfloat16 [128, 1024, 4096], P(('seq', 'grp')), may hold values from -0.1875 to 0.1875
- expert_down: bfloat16 [128, 4096, 1024], P(('seq', 'grp')), may hold values from -0.09375 to 0.09375
Outputs:
- block_out: bfloat16 [16384, 1024], P(('grp', 'seq'))
The draws below stay inside these ranges and needn't reach their ends.
Inputs may be any that keep to these rules, and one draw needn't show every extreme that they name: For the tokens of one device, no expert is named by more than 4 of their routes. `lengths`: some user has all 4096 behaviors valid in every draw.
All inputs are finite; a program needn't handle non-finite values.
Results may differ from the reference program's by a relative error of at most 0.0065.
Values may be sent and summed in bfloat16 or wider, within the bound.
A program may use at most 128 MiB of HBM per device.

```python
import math
import jax
import jax.numpy as jnp
import numpy as np
from jax import lax

D = 1024
HEADS = 8
HEAD_DIM = 128
FF = 4096
TOP = 2
USR_GRP = 2
TOK_DEV = 128
CAP = 4
USERS = 16
HIST = 4096
TOKENS = 16384
EXPERTS = 128


def user_table(key):
    return jax.random.randint(jax.random.fold_in(key, 71), (TOKENS,), 0, USR_GRP).astype(jnp.int32)


def key_table(key):
    return jax.random.truncated_normal(jax.random.fold_in(key, 72), -6.0, 6.0, (USERS, HIST, D), jnp.float32)


def draw_behavior_keys(key, part):
    table = key_table(key)
    return table.astype(jnp.bfloat16)


def draw_queries(key, part):
    rows = jax.random.truncated_normal(jax.random.fold_in(key, 76), -6.0, 6.0, (TOKENS, D), jnp.float32)
    return rows.astype(jnp.bfloat16)


def draw_user_of(key, part):
    return user_table(key)


def draw_lengths(key, part):
    drawn = jax.random.randint(jax.random.fold_in(key, 77), (USERS,), HIST // 4, HIST + 1).astype(jnp.int32)
    fullest = jax.random.randint(jax.random.fold_in(key, 78), (), 0, USERS).astype(jnp.int32)
    return drawn.at[fullest].set(HIST)


def block_levels(own_key, extent, cuts, smallest, top_value):
    factor_of = 1.0
    for position, shards_of in cuts:
        steps = jax.random.uniform(jax.random.fold_in(jax.random.fold_in(own_key, 6), position), (shards_of,), jnp.float32, smallest / len(cuts), top_value / len(cuts))
        factor_of = factor_of * jnp.repeat(jnp.exp(steps), extent[position] // shards_of).reshape((-1,) + (1,) * (len(extent) - 1 - position))
    return factor_of


def routed_block(key, own, number, rows, amount, top, bound, skew):
    order = jax.random.permutation(key, amount)
    crowded, usual = portions_of(amount, rows * top, bound, skew, True), portions_of(amount, rows * top, bound, skew, False)
    places = jnp.arange(amount)

    def named(sizes, offset_by):
        used = int((sizes > 0).sum())
        fixed = max(1, used // 4)
        passed = fixed + (places - fixed + offset_by * (used - fixed)) % max(1, amount - fixed)
        return jnp.zeros((amount,), jnp.int32).at[order[jnp.where(places < fixed, places, passed)]].set(jnp.asarray(sizes, jnp.int32))

    sizes = jnp.where(number % 4 == 0, named(crowded, number // 4), named(usual, number - number // 4 - 1))
    mixed = jax.random.permutation(jax.random.fold_in(own, 3), amount)
    source_of, sink = mixed[0:amount // 2 * 2:2], mixed[1:amount // 2 * 2:2]
    margin = jnp.minimum(sizes[source_of] - 1, bound - sizes[sink]) // 2
    margin = jnp.where((source_of == order[0]) | (sink == order[0]) | (sizes[sink] == 0), 0, jnp.maximum(margin, 0))
    passed = jax.random.randint(jax.random.fold_in(own, 4), (amount // 2,), 0, 1 << 20) % (margin + 1)
    sizes = sizes.at[source_of].add(-passed).at[sink].add(passed)
    items = jnp.searchsorted(jnp.cumsum(sizes), jnp.arange(rows * top), side="right").astype(jnp.int32)
    table = items.reshape(top, rows).T
    table = table[jax.random.permutation(jax.random.fold_in(own, 1), rows)]
    offset_by = jax.random.randint(jax.random.fold_in(own, 2), (rows, 1), 0, top)
    return jnp.take_along_axis(table, (jnp.arange(top)[None, :] + offset_by) % top, axis=1)


def portions_of(number_of, total, most, lean, full):
    weights = [(1 << 20) // math.isqrt(rank ** lean) + 1 for rank in range(1, number_of + 1)]
    largest = most if full else min(most, max(-(-total // number_of), total * weights[0] // sum(weights)))
    least = 1 if total - largest >= number_of - 1 else 0
    holding, rest = [largest] + [least] * (number_of - 1), total - largest - least * (number_of - 1)
    while rest > 0:
        movable = [i for i in range(1, number_of) if holding[i] < largest] or [i for i in range(1, number_of) if holding[i] < most]
        whole, budget = sum([weights[i] for i in movable]), rest
        for i in movable:
            more = min(most - holding[i], max(1, budget * weights[i] // whole), rest)
            holding[i] = holding[i] + more
            rest = rest - more
    return np.array(holding)


def centred(key, shape, scale, most, shards=(), held_as=jnp.bfloat16):
    factor_of = block_levels(key, shape, shards, -0.22, 0.18) if shards else 1.0
    values = jax.random.normal(key, shape, jnp.float32) * scale * factor_of
    return jnp.minimum(jnp.maximum(values, -most), most).astype(held_as)


def setup_inputs(seed: int = 0) -> dict:
    key_list = jax.random.split(jax.random.key(seed), 13)
    queries = draw_queries(jax.random.fold_in(key_list[12], 71), 0)
    states = centred(key_list[1], (TOKENS, D), 1.0, 6.0, ((0, 128),))
    behavior_keys = draw_behavior_keys(jax.random.fold_in(key_list[12], 71), 0)
    behavior_values = centred(key_list[3], (USERS, HIST, D), 1.0, 6.0, ((0, 8), (1, 16)))
    lengths = draw_lengths(jax.random.fold_in(key_list[12], 71), 0)
    user_of = draw_user_of(jax.random.fold_in(key_list[12], 71), 0)
    out_weight = centred(key_list[6], (D, D), D ** -0.5, 0.1875)
    norm_gain = jnp.clip(1.0 + 0.18 * jax.random.normal(key_list[7], (D,), jnp.float32), 0.1, 1.9)
    routes_keys = jax.random.split(jax.random.fold_in(key_list[8], 1), TOKENS // (TOK_DEV * TOP))
    routes_turns = jax.random.permutation(jax.random.fold_in(key_list[8], 3), TOKENS // (TOK_DEV * TOP))
    routes = jax.vmap(lambda own, number: routed_block(jax.random.fold_in(key_list[8], 2), own, number, TOK_DEV * TOP, EXPERTS, TOP, CAP, 2))(routes_keys, routes_turns).reshape((TOKENS, TOP))
    route_weights = jnp.clip(jnp.exp(math.log(1.0) - 1.3862944 * jax.random.uniform(key_list[9], (TOKENS, TOP), jnp.float32) ** block_levels(key_list[9], (TOKENS, TOP), ((0, 128),), -0.2, 0.2)), 0.25, 1.0)
    expert_up = centred(key_list[10], (EXPERTS, D, FF), D ** -0.5, 0.1875, ((0, 128),))
    expert_down = centred(key_list[11], (EXPERTS, FF, D), FF ** -0.5, 0.09375, ((0, 128),))
    return {"queries": queries, "states": states, "behavior_keys": behavior_keys, "behavior_values": behavior_values, "lengths": lengths, "user_of": user_of, "out_weight": out_weight, "norm_gain": norm_gain, "routes": routes, "route_weights": route_weights, "expert_up": expert_up, "expert_down": expert_down}


def attend_group(query_rows, owners, key_rows, value_rows, lengths):
    count = query_rows.shape[0]
    query_heads = query_rows.reshape(count, HEADS, HEAD_DIM).astype(jnp.float32)
    key_heads = key_rows.reshape(USR_GRP, HIST, HEADS, HEAD_DIM).astype(jnp.float32)
    value_heads = value_rows.reshape(USR_GRP, HIST, HEADS, HEAD_DIM).astype(jnp.float32)
    positions = jnp.arange(HIST, dtype=jnp.int32)
    factor = 1.0 / math.sqrt(HEAD_DIM)
    listing = []
    for member in range(USR_GRP):
        scores = jnp.einsum('ghd,phd->ghp', query_heads, key_heads[member]) * factor
        usable = (owners == member)[:, None, None] & (positions < lengths[member])[None, None, :]
        listing.append((jnp.where(usable, scores, -1e+30), usable))
    peaks = listing[0][0].max(-1)
    for scores, usable in listing[1:]:
        peaks = jnp.maximum(peaks, scores.max(-1))
    numer = jnp.zeros((count, HEADS, HEAD_DIM), jnp.float32)
    denom = jnp.zeros((count, HEADS), jnp.float32)
    for member in range(USR_GRP):
        scores, usable = listing[member]
        probs = jnp.where(usable, jnp.exp(scores - peaks[..., None]), 0.0)
        denom = denom + probs.sum(-1)
        low = probs.astype(jnp.bfloat16).astype(jnp.float32)
        numer = numer + jnp.einsum('ghp,phd->ghd', low, value_heads[member])
    return (numer / denom[..., None]).reshape(count, D).astype(jnp.bfloat16)

def expert_apply(rows, up_matrix, down_matrix):
    hidden = jax.nn.gelu(jnp.dot(rows, up_matrix, preferred_element_type=jnp.float32)).astype(jnp.bfloat16)
    return jnp.dot(hidden, down_matrix, preferred_element_type=jnp.float32).astype(jnp.bfloat16)

def reference(queries, states, behavior_keys, behavior_values, lengths, user_of, out_weight, norm_gain, routes, route_weights, expert_up, expert_down):
    groups = USERS // USR_GRP
    per_group = TOKENS // groups
    attended = lax.map(lambda packed: attend_group(*packed), (queries.reshape(groups, per_group, D), user_of.reshape(groups, per_group), behavior_keys.reshape(groups, USR_GRP, HIST, D), behavior_values.reshape(groups, USR_GRP, HIST, D), lengths.reshape(groups, USR_GRP)))
    attended = attended.reshape(TOKENS, D)
    residual = states.astype(jnp.float32) + jnp.dot(attended, out_weight, preferred_element_type=jnp.float32)
    spread = lax.optimization_barrier(jnp.mean(residual * residual, axis=-1, keepdims=True))
    normed = (residual / jnp.sqrt(spread + 1e-06) * norm_gain).astype(jnp.bfloat16)
    blocks = TOKENS // TOK_DEV
    width = TOK_DEV * TOP
    flat = routes.reshape(blocks, width)
    onehot = (flat[:, :, None] == jnp.arange(EXPERTS, dtype=jnp.int32)[None, None, :]).astype(jnp.int32)
    earlier = jnp.cumsum(onehot, axis=1) - onehot
    slots = lax.optimization_barrier(jnp.sum(earlier * onehot, axis=2))
    block_ids = jnp.arange(blocks, dtype=jnp.int32)[:, None]
    target = (flat * (blocks * CAP) + block_ids * CAP + slots).reshape(-1).astype(jnp.int32)
    rows = jnp.broadcast_to(normed[:, None, :], (TOKENS, TOP, D)).reshape(-1, D)
    buffer = jnp.zeros((EXPERTS * blocks * CAP, D), jnp.bfloat16).at[target].set(rows)
    buffer = buffer.reshape(EXPERTS, blocks * CAP, D)
    answered = lax.map(lambda packed: expert_apply(*packed), (buffer, expert_up, expert_down))
    picked = answered.reshape(-1, D)[target].astype(jnp.float32).reshape(TOKENS, TOP, D)
    mixed = lax.optimization_barrier(jnp.sum(picked * route_weights[:, :, None], axis=1))
    return (residual + mixed).astype(jnp.bfloat16)
```

```python
import functools
import math

import jax
import jax.numpy as jnp
from jax import lax
from jax.experimental import pallas as pl
from jax.experimental.pallas import tpu as pltpu
from jax.sharding import PartitionSpec as P

HEADS = 8
MESH = pl.DeviceIdType.MESH
BF = jnp.bfloat16
F32 = jnp.float32
LOW = -1e30

FULL = ((0, 1), (0, 3), (1, 0), (3, 0))
FIRST = ((1, 1), (1, 3), (2, 0))
SECOND = ((3, 3), (3, 1), (0, 2))
HALVES = FIRST + SECOND


def head_of(y, z):
    return (y % 2) * 4 + (z + 2 * (y // 2)) % 4


def seq_of(y, z):
    return ((y + 8) % 4) * 4 + (z + 8) % 4


def cols(head, width=128):
    return pl.ds(pl.multiple_of(head * width, width), width)


def attention_kernel(
    q_hbm, k_hbm, v_hbm, len_ref, user_ref, routes_ref,
    att_ref, partner_ref,
    q_v, k_v, v_v, qbuf, kcat, vcat, qt, score, prob, osend, obuf, ssend, sbuf, rbuf,
    load_sem, own_sem, qs, qr, ks, kr, vs, vr, os, orr, ss, sr, rs, rr,
):
    me = lax.axis_index("seq")
    y, z = me // 4, me % 4
    head = head_of(y, z)
    hist = k_hbm.shape[1]
    half = hist // 2
    tok = q_hbm.shape[0]
    count = 16
    width = 128
    scale = math.log2(math.e) / math.sqrt(width)

    loads = [
        pltpu.make_async_copy(src, dst, load_sem.at[i])
        for i, (src, dst) in enumerate(((q_hbm, q_v), (k_hbm, k_v), (v_hbm, v_v)))
    ]
    for copy in loads:
        copy.start()
    own = [pltpu.make_async_copy(q_hbm.at[:, cols(head)], qbuf.at[me], own_sem.at[0])]
    for i, (src, dst) in enumerate(((k_hbm, kcat), (v_hbm, vcat))):
        for user in range(2):
            own.append(
                pltpu.make_async_copy(
                    src.at[user, :, cols(head)],
                    dst.at[pl.ds(0, hist), pl.ds(user * width, width)],
                    own_sem.at[1 + 2 * i + user],
                )
            )
    for copy in own:
        copy.start()

    barrier = pltpu.get_barrier_semaphore()
    for step in range(1, count):
        pl.semaphore_signal(
            barrier, inc=1, device_id={"seq": (me + step) % count}, device_id_type=MESH
        )
    pl.semaphore_wait(barrier, count - 1)

    partner = me + 1 - 2 * (me % 2)
    route_copy = pltpu.make_async_remote_copy(
        src_ref=routes_ref, dst_ref=rbuf, send_sem=rs, recv_sem=rr,
        device_id={"seq": partner}, device_id_type=MESH,
    )
    route_copy.start()

    loads[0].wait()
    for dy in range(4):
        for dz in range(4):
            if dy == 0 and dz == 0:
                continue
            ty, tz = (y + dy) % 4, (z + dz) % 4
            pltpu.make_async_remote_copy(
                src_ref=q_v.at[:, cols(head_of(ty, tz))],
                dst_ref=qbuf.at[me],
                send_sem=qs, recv_sem=qr,
                device_id={"seq": ty * 4 + tz}, device_id_type=MESH,
            ).start()

    def send_rows(src, dst, send_sem, recv_sem):
        for j, (dy, dz) in enumerate(HALVES):
            ty, tz = (y - dy + 4) % 4, (z - dz + 4) % 4
            first = 0 if (dy, dz) in FIRST else half
            for user in range(2):
                pltpu.make_async_remote_copy(
                    src_ref=src.at[user, pl.ds(first, half), cols(head_of(ty, tz))],
                    dst_ref=dst.at[pl.ds(5 * hist + j * half, half), pl.ds(user * width, width)],
                    send_sem=send_sem, recv_sem=recv_sem,
                    device_id={"seq": ty * 4 + tz}, device_id_type=MESH,
                ).start()
        for j, (dy, dz) in enumerate(FULL):
            ty, tz = (y - dy + 4) % 4, (z - dz + 4) % 4
            for user in range(2):
                pltpu.make_async_remote_copy(
                    src_ref=src.at[user, :, cols(head_of(ty, tz))],
                    dst_ref=dst.at[pl.ds((1 + j) * hist, hist), pl.ds(user * width, width)],
                    send_sem=send_sem, recv_sem=recv_sem,
                    device_id={"seq": ty * 4 + tz}, device_id_type=MESH,
                ).start()

    loads[1].wait()
    send_rows(k_v, kcat, ks, kr)
    loads[2].wait()
    send_rows(v_v, vcat, vs, vr)

    starts = []
    for dy, dz in ((0, 0),) + FULL:
        base = seq_of(y + dy, z + dz) * hist
        starts += [base, base + half]
    for dy, dz in HALVES:
        base = seq_of(y + dy, z + dz) * hist
        starts.append(base if (dy, dz) in FIRST else base + half)

    own[0].wait()
    moved = pl.ds(0, count - 1)
    pltpu.make_async_copy(qbuf.at[moved], qbuf.at[moved], qr).wait()
    for i in range(count):
        flipped = qbuf[i].T
        users = user_ref[:, i * tok : (i + 1) * tok]
        for user in range(2):
            qt[user * width : (user + 1) * width, i * tok : (i + 1) * tok] = jnp.where(
                users == user, flipped, jnp.zeros_like(flipped)
            )

    rest = pl.ds(hist, kcat.shape[0] - hist)
    own[1].wait()
    own[2].wait()
    pltpu.make_async_copy(kcat.at[rest], kcat.at[rest], kr).wait()

    tokens = count * tok
    block = 4 * tok
    limit0 = len_ref[0, 0]
    limit1 = len_ref[0, 1]
    stat = {}
    for b in range(tokens // block):
        here = pl.ds(b * block, block)
        users = user_ref[:, b * block : (b + 1) * block]
        limit = jnp.where(users == 0, limit0, limit1)
        top = jnp.full((8, block), LOW, F32)
        for c, start in enumerate(starts):
            s = jnp.dot(kcat[c * half : (c + 1) * half, :], qt[:, here], preferred_element_type=F32)
            pos = start + lax.broadcasted_iota(jnp.int32, (half, block), 0)
            s = jnp.where(pos < limit, s, LOW)
            score[c * half : (c + 1) * half, :] = s
            top = jnp.maximum(top, s.reshape(half // 8, 8, block).max(0))
        peak = top.max(0, keepdims=True)
        total = jnp.zeros((8, block), F32)
        for c in range(len(starts)):
            p = jnp.exp2((score[c * half : (c + 1) * half, :] - peak) * scale)
            total = total + p.reshape(half // 8, 8, block).sum(0)
            prob[c * half : (c + 1) * half, here] = p.astype(BF)
        stat[b] = (peak, total.sum(0, keepdims=True))

    own[3].wait()
    own[4].wait()
    pltpu.make_async_copy(vcat.at[rest], vcat.at[rest], vr).wait()

    for b in range(tokens // block):
        here = pl.ds(b * block, block)
        users = user_ref[:, b * block : (b + 1) * block]
        both = lax.dot_general(
            vcat[...], prob[:, here], (((0,), (0,)), ((), ())), preferred_element_type=F32
        )
        peak, total = stat[b]
        out = jnp.where(users == 0, both[:width], both[width:]) * (1.0 / total)
        out = out.astype(BF)
        packed = jnp.concatenate([peak, total, jnp.zeros((6, block), F32)], axis=0)
        for i in range(block // tok):
            owner = b * (block // tok) + i
            osend[owner] = out[:, i * tok : (i + 1) * tok]
            ssend[owner] = packed[:, i * tok : (i + 1) * tok]
        for i in range(block // tok):
            owner = b * (block // tok) + i

            @pl.when(owner != me)
            def _(owner=owner):
                pltpu.make_async_remote_copy(
                    src_ref=osend.at[owner], dst_ref=obuf.at[me], send_sem=os, recv_sem=orr,
                    device_id={"seq": owner}, device_id_type=MESH,
                ).start()
                pltpu.make_async_remote_copy(
                    src_ref=ssend.at[owner], dst_ref=sbuf.at[me], send_sem=ss, recv_sem=sr,
                    device_id={"seq": owner}, device_id_type=MESH,
                ).start()

    obuf[me] = osend[me]
    sbuf[me] = ssend[me]
    route_copy.wait()
    partner_ref[...] = rbuf[...]
    pltpu.make_async_copy(qbuf.at[moved], qbuf.at[moved], qs).wait()
    pltpu.make_async_copy(kcat.at[rest], kcat.at[rest], ks).wait()
    pltpu.make_async_copy(vcat.at[rest], vcat.at[rest], vs).wait()
    pltpu.make_async_copy(obuf.at[moved], obuf.at[moved], os).wait()
    pltpu.make_async_copy(sbuf.at[moved], sbuf.at[moved], ss).wait()
    pltpu.make_async_copy(obuf.at[moved], obuf.at[moved], orr).wait()
    pltpu.make_async_copy(sbuf.at[moved], sbuf.at[moved], sr).wait()

    for h in range(HEADS):
        hy, hz = h // 4, h % 4
        first = hy * 4 + hz
        second = (hy + 2) * 4 + (hz + 2) % 4
        m0, d0 = sbuf[first, 0:1], sbuf[first, 1:2]
        m1, d1 = sbuf[second, 0:1], sbuf[second, 1:2]
        top = jnp.maximum(m0, m1)
        w0 = d0 * jnp.exp2((m0 - top) * scale)
        w1 = d1 * jnp.exp2((m1 - top) * scale)
        inverse = 1.0 / (w0 + w1)
        merged = obuf[first].astype(F32) * (w0 * inverse) + obuf[second].astype(F32) * (w1 * inverse)
        att_ref[h * width : (h + 1) * width, :] = merged.astype(BF)


def attention(queries, keys, values, lengths, users, routes):
    tok, model = queries.shape
    hist = keys.shape[1]
    width = model // HEADS
    rows = 8 * hist
    count = 16
    any_spec = pl.BlockSpec(memory_space=pl.ANY)
    vmem = pl.BlockSpec(memory_space=pltpu.VMEM)
    smem = pl.BlockSpec(memory_space=pltpu.SMEM)
    dma = pltpu.SemaphoreType.DMA
    return pl.pallas_call(
        attention_kernel,
        out_shape=(
            jax.ShapeDtypeStruct((model, tok), BF),
            jax.ShapeDtypeStruct((2, tok), jnp.int32),
        ),
        in_specs=[any_spec, any_spec, any_spec, smem, vmem, vmem],
        out_specs=(vmem, vmem),
        scratch_shapes=[
            pltpu.VMEM((tok, model), BF),
            pltpu.VMEM((2, hist, model), BF),
            pltpu.VMEM((2, hist, model), BF),
            pltpu.VMEM((count, tok, width), BF),
            pltpu.VMEM((rows, 2 * width), BF),
            pltpu.VMEM((rows, 2 * width), BF),
            pltpu.VMEM((2 * width, count * tok), BF),
            pltpu.VMEM((rows, 4 * tok), F32),
            pltpu.VMEM((rows, count * tok), BF),
            pltpu.VMEM((count, width, tok), BF),
            pltpu.VMEM((count, width, tok), BF),
            pltpu.VMEM((count, 8, tok), F32),
            pltpu.VMEM((count, 8, tok), F32),
            pltpu.VMEM((2, tok), jnp.int32),
            dma((3,)),
            dma((5,)),
        ]
        + [dma] * 12,
        compiler_params=pltpu.CompilerParams(
            collective_id=0, has_side_effects=True, vmem_limit_bytes=48 * 1024 * 1024
        ),
        name="attention",
    )(queries, keys, values, lengths, users, routes)


def experts_kernel(
    att_ref, partner_ref, routes_ref, gates_ref, states_ref, gain_ref, wo_hbm, up_hbm, down_hbm,
    out_ref,
    wo, up, down, send, recv, hidden, back, answer,
    load_sem, ds, dr, bs, br,
):
    s, g = lax.axis_index("seq"), lax.axis_index("grp")
    seqs, grps = 16, 8
    total = seqs * grps
    me = s * grps + g
    parity = s % 2
    pair = g * (seqs // 2) + s // 2
    tok, model = states_ref.shape
    ff = up.shape[1]
    loads = [
        pltpu.make_async_copy(src, dst, load_sem.at[i])
        for i, (src, dst) in enumerate(((wo_hbm, wo), (up_hbm.at[0], up), (down_hbm.at[0], down)))
    ]
    for copy in loads:
        copy.start()

    barrier = pltpu.get_barrier_semaphore()

    def greet(i, carry):
        other = (me + i) % total
        pl.semaphore_signal(
            barrier, inc=1, device_id={"seq": other // grps, "grp": other % grps},
            device_id_type=MESH,
        )
        return carry

    lax.fori_loop(1, total, greet, 0)

    experts = lax.broadcasted_iota(jnp.int32, (total, tok), 0)
    named = [(routes_ref[k : k + 1, :] == experts).astype(F32) for k in range(2)]
    others = sum((partner_ref[k : k + 1, :] == experts).astype(F32) for k in range(2))
    earlier = (
        lax.broadcasted_iota(jnp.int32, (tok, tok), 0) < lax.broadcasted_iota(jnp.int32, (tok, tok), 1)
    ).astype(BF)
    rank = jnp.dot((named[0] + named[1]).astype(BF), earlier, preferred_element_type=F32)
    ahead = jnp.dot(others.astype(BF), jnp.ones((tok, tok), BF), preferred_element_type=F32)
    rank = rank + ahead * parity.astype(F32)
    places = lax.broadcasted_iota(jnp.int32, (4 * total, tok), 0)
    onehot = []
    for k in range(2):
        slot = jnp.sum(named[k] * rank, axis=0, keepdims=True).astype(jnp.int32)
        target = routes_ref[k : k + 1, :] * 4 + slot
        onehot.append((places == target).astype(F32).astype(BF))
    placed = onehot[0] + onehot[1]

    loads[0].wait()
    residual = states_ref[...].astype(F32) + lax.dot_general(
        att_ref[...], wo[...], (((0,), (0,)), ((), ())), preferred_element_type=F32
    )
    spread = jnp.mean(residual * residual, axis=-1, keepdims=True)
    normed = (residual / jnp.sqrt(spread + 1e-06) * gain_ref[...]).astype(BF)
    send[...] = (
        jnp.dot(placed, normed, preferred_element_type=F32).reshape(total, 4, model).astype(BF)
    )

    pl.semaphore_wait(barrier, total - 1)

    def dispatch(i, carry):
        other = (me + i) % total
        pltpu.make_async_remote_copy(
            src_ref=send.at[other], dst_ref=recv.at[parity, pair], send_sem=ds, recv_sem=dr,
            device_id={"seq": other // grps, "grp": other % grps}, device_id_type=MESH,
        ).start()
        return carry

    lax.fori_loop(1, total, dispatch, 0)
    recv[parity, pair] = send[me]
    loads[1].wait()
    loads[2].wait()
    moved = pl.ds(0, total - 1)
    pltpu.make_async_copy(answer.at[moved], answer.at[moved], dr).wait()
    rows = (recv[0].astype(F32) + recv[1].astype(F32)).reshape(2 * total, model).astype(BF)
    step = 512
    for j in range(ff // step):
        hidden[:, j * step : (j + 1) * step] = jax.nn.gelu(
            jnp.dot(rows, up[:, j * step : (j + 1) * step], preferred_element_type=F32)
        ).astype(BF)
    step = 256
    for j in range(model // step):
        back[:, :, j * step : (j + 1) * step] = (
            jnp.dot(hidden[...], down[:, j * step : (j + 1) * step], preferred_element_type=F32)
            .reshape(total // 2, 4, step)
            .astype(BF)
        )

    def reply(i, carry):
        other = (me + i) % total
        os, og = other // grps, other % grps
        pltpu.make_async_remote_copy(
            src_ref=back.at[og * (seqs // 2) + os // 2], dst_ref=answer.at[me],
            send_sem=bs, recv_sem=br,
            device_id={"seq": os, "grp": og}, device_id_type=MESH,
        ).start()
        return carry

    lax.fori_loop(1, total, reply, 0)
    answer[me] = back[pair]
    pltpu.make_async_copy(answer.at[moved], answer.at[moved], ds).wait()
    pltpu.make_async_copy(answer.at[moved], answer.at[moved], bs).wait()
    pltpu.make_async_copy(answer.at[moved], answer.at[moved], br).wait()
    answers = answer[...].astype(F32).reshape(4 * total, model).astype(BF)
    mixed = residual
    for k in range(2):
        picked = lax.dot_general(
            onehot[k], answers, (((0,), (0,)), ((), ())), preferred_element_type=F32
        )
        mixed = mixed + picked * gates_ref[:, k : k + 1]
    out_ref[...] = mixed.astype(BF)


def experts(att, partner, routes, gates, states, gain, out_weight, up, down):
    tok, model = states.shape
    ff = up.shape[2]
    total = 128
    any_spec = pl.BlockSpec(memory_space=pl.ANY)
    vmem = pl.BlockSpec(memory_space=pltpu.VMEM)
    dma = pltpu.SemaphoreType.DMA
    return pl.pallas_call(
        experts_kernel,
        out_shape=jax.ShapeDtypeStruct((tok, model), BF),
        in_specs=[vmem] * 6 + [any_spec] * 3,
        out_specs=vmem,
        scratch_shapes=[
            pltpu.VMEM((model, model), BF),
            pltpu.VMEM((model, ff), BF),
            pltpu.VMEM((ff, model), BF),
            pltpu.VMEM((total, 4, model), BF),
            pltpu.VMEM((2, total // 2, 4, model), BF),
            pltpu.VMEM((2 * total, ff), BF),
            pltpu.VMEM((total // 2, 4, model), BF),
            pltpu.VMEM((total, 4, model), BF),
            dma((3,)),
        ]
        + [dma] * 4,
        compiler_params=pltpu.CompilerParams(
            collective_id=1, has_side_effects=True, vmem_limit_bytes=56 * 1024 * 1024
        ),
        name="experts",
    )(att, partner, routes, gates, states, gain, out_weight, up, down)


def body(
    queries, states, behavior_keys, behavior_values, lengths, user_of, out_weight, norm_gain,
    routes, route_weights, expert_up, expert_down,
):
    routes_t = routes.T
    att, partner = attention(
        queries, behavior_keys, behavior_values, lengths.reshape(1, -1), user_of.reshape(1, -1),
        routes_t,
    )
    return experts(
        att, partner, routes_t, route_weights, states, norm_gain.reshape(1, -1), out_weight,
        expert_up, expert_down,
    )


def solution(mesh):
    return jax.shard_map(
        body,
        mesh=mesh,
        in_specs=(
            P(("grp", "seq"), None),
            P(("grp", "seq"), None),
            P("grp", "seq", None),
            P("grp", "seq", None),
            P("grp"),
            P("grp"),
            P(),
            P(),
            P(("grp", "seq"), None),
            P(("grp", "seq"), None),
            P(("seq", "grp"), None, None),
            P(("seq", "grp"), None, None),
        ),
        out_specs=P(("grp", "seq"), None),
        check_vma=False,
    )
```

```python
import itertools
import math

import jax
import jax.numpy as jnp
from jax import lax
from jax.experimental import pallas as pl
from jax.experimental.pallas import tpu as pltpu
from jax.sharding import PartitionSpec as P

HEADS = 8
MESH = pl.DeviceIdType.MESH
BF = jnp.bfloat16
F32 = jnp.float32
LOW = -1e30
VMEM_ALL = 67043328

FULL = ((0, 1), (0, 3), (1, 0), (3, 0))
FIRST = ((1, 1), (1, 3), (2, 0))
SECOND = ((3, 3), (3, 1), (0, 2))
HALVES = FIRST + SECOND


def head_of(y, z):
    return (y % 2) * 4 + (z + 2 * (y // 2)) % 4


def seq_of(y, z):
    return ((y + 8) % 4) * 4 + (z + 8) % 4


def far_first(steps):
    def hops(step):
        return sum(min(d, 4 - d) for d in step[:3])

    return sorted((s for s in steps if any(s)), key=lambda s: (-hops(s), sum(s) % 3, s))


def cols(head, width=128):
    return pl.ds(pl.multiple_of(head * width, width), width)


def attention_kernel(
    q_hbm, k_hbm, v_hbm, len_hbm, user_hbm, routes_hbm,
    att_ref, partner_ref,
    len_ref, user_ref, routes_ref, q_v, k_v, v_v, qbuf, kcat, vcat, qt, score, prob, osend, obuf, ssend, sbuf, rbuf,
    load_sem, own_sem, qs, qr, ks, kr, vs, vr, os, orr, ss, sr, rs, rr,
):
    me = lax.axis_index("seq")
    y, z = me // 4, me % 4
    head = head_of(y, z)
    hist = k_hbm.shape[1]
    half = hist // 2
    tok = q_hbm.shape[0]
    count = 16
    width = 128
    scale = math.log2(math.e) / math.sqrt(width)

    loads = [
        pltpu.make_async_copy(src, dst, load_sem.at[i])
        for i, (src, dst) in enumerate(
            (
                (q_hbm, q_v), (k_hbm, k_v), (v_hbm, v_v),
                (routes_hbm, routes_ref), (user_hbm, user_ref), (len_hbm, len_ref),
            )
        )
    ]
    for copy in loads:
        copy.start()
    own = [pltpu.make_async_copy(q_hbm.at[:, cols(head)], qbuf.at[me], own_sem.at[0])]
    for i, (src, dst) in enumerate(((k_hbm, kcat), (v_hbm, vcat))):
        for user in range(2):
            own.append(
                pltpu.make_async_copy(
                    src.at[user, :, cols(head)],
                    dst.at[pl.ds(0, hist), pl.ds(user * width, width)],
                    own_sem.at[1 + 2 * i + user],
                )
            )
    for copy in own:
        copy.start()

    barrier = pltpu.get_barrier_semaphore()
    for step in range(1, count):
        pl.semaphore_signal(
            barrier, inc=1, device_id={"seq": (me + step) % count}, device_id_type=MESH
        )
    pl.semaphore_wait(barrier, count - 1)

    partner = me + 1 - 2 * (me % 2)
    loads[3].wait()
    route_copy = pltpu.make_async_remote_copy(
        src_ref=routes_ref, dst_ref=rbuf, send_sem=rs, recv_sem=rr,
        device_id={"seq": partner}, device_id_type=MESH,
    )
    loads[0].wait()
    for dy, dz in far_first(itertools.product(range(4), range(4))):
        ty, tz = (y + dy) % 4, (z + dz) % 4
        pltpu.make_async_remote_copy(
            src_ref=q_v.at[:, cols(head_of(ty, tz))],
            dst_ref=qbuf.at[me],
            send_sem=qs, recv_sem=qr,
            device_id={"seq": ty * 4 + tz}, device_id_type=MESH,
        ).start()
    route_copy.start()

    def send_rows(src, dst, send_sem, recv_sem):
        for j, (dy, dz) in enumerate(HALVES):
            ty, tz = (y - dy + 4) % 4, (z - dz + 4) % 4
            first = 0 if (dy, dz) in FIRST else half
            for user in range(2):
                pltpu.make_async_remote_copy(
                    src_ref=src.at[user, pl.ds(first, half), cols(head_of(ty, tz))],
                    dst_ref=dst.at[pl.ds(5 * hist + j * half, half), pl.ds(user * width, width)],
                    send_sem=send_sem, recv_sem=recv_sem,
                    device_id={"seq": ty * 4 + tz}, device_id_type=MESH,
                ).start()
        for j, (dy, dz) in enumerate(FULL):
            ty, tz = (y - dy + 4) % 4, (z - dz + 4) % 4
            for user in range(2):
                pltpu.make_async_remote_copy(
                    src_ref=src.at[user, :, cols(head_of(ty, tz))],
                    dst_ref=dst.at[pl.ds((1 + j) * hist, hist), pl.ds(user * width, width)],
                    send_sem=send_sem, recv_sem=recv_sem,
                    device_id={"seq": ty * 4 + tz}, device_id_type=MESH,
                ).start()

    loads[1].wait()
    send_rows(k_v, kcat, ks, kr)
    loads[2].wait()
    send_rows(v_v, vcat, vs, vr)

    starts = []
    for dy, dz in ((0, 0),) + FULL:
        base = seq_of(y + dy, z + dz) * hist
        starts += [base, base + half]
    for dy, dz in HALVES:
        base = seq_of(y + dy, z + dz) * hist
        starts.append(base if (dy, dz) in FIRST else base + half)

    loads[4].wait()
    loads[5].wait()
    own[0].wait()
    moved = pl.ds(0, count - 1)
    pltpu.make_async_copy(qbuf.at[moved], qbuf.at[moved], qr).wait()
    for i in range(count):
        flipped = qbuf[i].T
        users = user_ref[:, i * tok : (i + 1) * tok]
        for user in range(2):
            qt[user * width : (user + 1) * width, i * tok : (i + 1) * tok] = jnp.where(
                users == user, flipped, jnp.zeros_like(flipped)
            )

    rest = pl.ds(hist, kcat.shape[0] - hist)
    own[1].wait()
    own[2].wait()
    pltpu.make_async_copy(kcat.at[rest], kcat.at[rest], kr).wait()

    tokens = count * tok
    block = 4 * tok
    limit0 = len_ref[0:1, 0:1]
    limit1 = len_ref[0:1, 1:2]
    stat = {}
    for b in range(tokens // block):
        here = pl.ds(b * block, block)
        users = user_ref[:, b * block : (b + 1) * block]
        limit = jnp.where(users == 0, limit0, limit1)
        top = jnp.full((8, block), LOW, F32)
        for c, start in enumerate(starts):
            s = jnp.dot(kcat[c * half : (c + 1) * half, :], qt[:, here], preferred_element_type=F32)
            pos = start + lax.broadcasted_iota(jnp.int32, (half, block), 0)
            s = jnp.where(pos < limit, s, LOW)
            score[c * half : (c + 1) * half, :] = s
            top = jnp.maximum(top, s.reshape(half // 8, 8, block).max(0))
        peak = top.max(0, keepdims=True)
        total = jnp.zeros((8, block), F32)
        for c in range(len(starts)):
            p = jnp.exp2((score[c * half : (c + 1) * half, :] - peak) * scale)
            total = total + p.reshape(half // 8, 8, block).sum(0)
            prob[c * half : (c + 1) * half, here] = p.astype(BF)
        stat[b] = (peak, total.sum(0, keepdims=True))

    own[3].wait()
    own[4].wait()
    pltpu.make_async_copy(vcat.at[rest], vcat.at[rest], vr).wait()

    for b in range(tokens // block):
        here = pl.ds(b * block, block)
        users = user_ref[:, b * block : (b + 1) * block]
        both = lax.dot_general(
            vcat[...], prob[:, here], (((0,), (0,)), ((), ())), preferred_element_type=F32
        )
        peak, total = stat[b]
        out = jnp.where(users == 0, both[:width], both[width:]) * (1.0 / total)
        out = out.astype(BF)
        packed = jnp.concatenate([peak, total, jnp.zeros((6, block), F32)], axis=0)
        for i in range(block // tok):
            owner = b * (block // tok) + i
            osend[owner] = out[:, i * tok : (i + 1) * tok]
            ssend[owner] = packed[:, i * tok : (i + 1) * tok]
        for i in range(block // tok):
            owner = b * (block // tok) + i

            @pl.when(owner != me)
            def _(owner=owner):
                pltpu.make_async_remote_copy(
                    src_ref=osend.at[owner], dst_ref=obuf.at[me], send_sem=os, recv_sem=orr,
                    device_id={"seq": owner}, device_id_type=MESH,
                ).start()
                pltpu.make_async_remote_copy(
                    src_ref=ssend.at[owner], dst_ref=sbuf.at[me], send_sem=ss, recv_sem=sr,
                    device_id={"seq": owner}, device_id_type=MESH,
                ).start()

    obuf[me] = osend[me]
    sbuf[me] = ssend[me]
    route_copy.wait()
    partner_ref[...] = rbuf[...]
    pltpu.make_async_copy(qbuf.at[moved], qbuf.at[moved], qs).wait()
    pltpu.make_async_copy(kcat.at[rest], kcat.at[rest], ks).wait()
    pltpu.make_async_copy(vcat.at[rest], vcat.at[rest], vs).wait()
    pltpu.make_async_copy(obuf.at[moved], obuf.at[moved], os).wait()
    pltpu.make_async_copy(sbuf.at[moved], sbuf.at[moved], ss).wait()
    pltpu.make_async_copy(obuf.at[moved], obuf.at[moved], orr).wait()
    pltpu.make_async_copy(sbuf.at[moved], sbuf.at[moved], sr).wait()

    for h in range(HEADS):
        hy, hz = h // 4, h % 4
        first = hy * 4 + hz
        second = (hy + 2) * 4 + (hz + 2) % 4
        m0, d0 = sbuf[first, 0:1], sbuf[first, 1:2]
        m1, d1 = sbuf[second, 0:1], sbuf[second, 1:2]
        top = jnp.maximum(m0, m1)
        w0 = d0 * jnp.exp2((m0 - top) * scale)
        w1 = d1 * jnp.exp2((m1 - top) * scale)
        inverse = 1.0 / (w0 + w1)
        merged = obuf[first].astype(F32) * (w0 * inverse) + obuf[second].astype(F32) * (w1 * inverse)
        att_ref[h * width : (h + 1) * width, :] = merged.astype(BF)


def attention(queries, keys, values, lengths, users, routes):
    tok, model = queries.shape
    hist = keys.shape[1]
    width = model // HEADS
    rows = 8 * hist
    count = 16
    hbm = pl.BlockSpec(memory_space=pltpu.HBM)
    vmem = pl.BlockSpec(memory_space=pltpu.VMEM)
    dma = pltpu.SemaphoreType.DMA
    return pl.pallas_call(
        attention_kernel,
        out_shape=(
            jax.ShapeDtypeStruct((model, tok), BF),
            jax.ShapeDtypeStruct((2, tok), jnp.int32),
        ),
        in_specs=[hbm] * 6,
        out_specs=(vmem, vmem),
        scratch_shapes=[
            pltpu.VMEM(lengths.shape, jnp.int32),
            pltpu.VMEM(users.shape, jnp.int32),
            pltpu.VMEM((2, tok), jnp.int32),
            pltpu.VMEM((tok, model), BF),
            pltpu.VMEM((2, hist, model), BF),
            pltpu.VMEM((2, hist, model), BF),
            pltpu.VMEM((count, tok, width), BF),
            pltpu.VMEM((rows, 2 * width), BF),
            pltpu.VMEM((rows, 2 * width), BF),
            pltpu.VMEM((2 * width, count * tok), BF),
            pltpu.VMEM((rows, 4 * tok), F32),
            pltpu.VMEM((rows, count * tok), BF),
            pltpu.VMEM((count, width, tok), BF),
            pltpu.VMEM((count, width, tok), BF),
            pltpu.VMEM((count, 8, tok), F32),
            pltpu.VMEM((count, 8, tok), F32),
            pltpu.VMEM((2, tok), jnp.int32),
            dma((6,)),
            dma((5,)),
        ]
        + [dma] * 12,
        compiler_params=pltpu.CompilerParams(
            collective_id=0, has_side_effects=True, vmem_limit_bytes=VMEM_ALL
        ),
        name="attention",
    )(queries, keys, values, lengths, users, routes)


def experts_kernel(
    att_hbm, partner_hbm, routes_hbm, gates_hbm, states_hbm, gain_hbm, wo_hbm, up_hbm, down_hbm,
    out_ref,
    att_ref, partner_ref, routes_ref, gates_ref, states_ref, gain_ref, wo, up, down,
    send, recv, partial, hidden, back, answer,
    load_sem, ds, dr, bs, br,
):
    s, g = lax.axis_index("seq"), lax.axis_index("grp")
    seqs, grps = 16, 8
    total = seqs * grps
    me = s * grps + g
    parity = s % 2
    pair = g * (seqs // 2) + s // 2
    tok, model = states_ref.shape
    ff = up.shape[1]
    parts = send.shape[0]
    part = model // parts
    loads = [
        pltpu.make_async_copy(src, dst, load_sem.at[i])
        for i, (src, dst) in enumerate(
            (
                (routes_hbm, routes_ref), (wo_hbm, wo), (states_hbm, states_ref),
                (gain_hbm, gain_ref), (gates_hbm, gates_ref),
                (up_hbm.at[0], up), (down_hbm.at[0], down),
                (att_hbm, att_ref), (partner_hbm, partner_ref),
            )
        )
    ]
    for i in (0, 8, 7, 1, 2, 3, 4, 5, 6):
        loads[i].start()

    barrier = pltpu.get_barrier_semaphore()

    def greet(i, carry):
        other = (me + i) % total
        pl.semaphore_signal(
            barrier, inc=1, device_id={"seq": other // grps, "grp": other % grps},
            device_id_type=MESH,
        )
        return carry

    lax.fori_loop(1, total, greet, 0)

    ys = [(s // 4 + d) % 4 * 4 for d in range(4)]
    zs = [(s + d) % 4 for d in range(4)]
    xs = [(g // 2 + d) % 4 * 2 for d in range(4)]
    cs = [(g + d) % 2 for d in range(2)]
    others = [
        (ys[dy] + zs[dz], xs[dx] + cs[dc])
        for dy, dz, dx, dc in far_first(itertools.product(range(4), range(4), range(4), range(2)))
    ]

    loads[0].wait()
    loads[8].wait()
    experts = lax.broadcasted_iota(jnp.int32, (total, tok), 0)
    named = [(routes_ref[k : k + 1, :] == experts).astype(F32) for k in range(2)]
    theirs = sum((partner_ref[k : k + 1, :] == experts).astype(F32) for k in range(2))
    earlier = (
        lax.broadcasted_iota(jnp.int32, (tok, tok), 0) < lax.broadcasted_iota(jnp.int32, (tok, tok), 1)
    ).astype(BF)
    rank = jnp.dot((named[0] + named[1]).astype(BF), earlier, preferred_element_type=F32)
    ahead = jnp.dot(theirs.astype(BF), jnp.ones((tok, tok), BF), preferred_element_type=F32)
    rank = rank + ahead * parity.astype(F32)
    places = lax.broadcasted_iota(jnp.int32, (4 * total, tok), 0)
    onehot = []
    for k in range(2):
        slot = jnp.sum(named[k] * rank, axis=0, keepdims=True).astype(jnp.int32)
        target = routes_ref[k : k + 1, :] * 4 + slot
        onehot.append((places == target).astype(F32).astype(BF))
    placed = onehot[0] + onehot[1]

    loads[7].wait()
    loads[1].wait()
    loads[2].wait()
    residual = states_ref[...].astype(F32) + lax.dot_general(
        att_ref[...], wo[...], (((0,), (0,)), ((), ())), preferred_element_type=F32
    )
    spread = jnp.mean(residual * residual, axis=-1, keepdims=True)
    loads[3].wait()
    normed = (residual / jnp.sqrt(spread + 1e-06) * gain_ref[...]).astype(BF)

    def whole(buffer):
        return buffer.at[pl.ds(0, total - 1)]

    for p in range(parts):
        send[p] = (
            jnp.dot(placed, normed[:, p * part : (p + 1) * part], preferred_element_type=F32)
            .reshape(total, 4, part)
            .astype(BF)
        )
        if p == 0:
            pl.semaphore_wait(barrier, total - 1)
        for os, og in others:
            pltpu.make_async_remote_copy(
                src_ref=send.at[p, os * grps + og], dst_ref=recv.at[p, parity, pair],
                send_sem=ds.at[p], recv_sem=dr.at[p],
                device_id={"seq": os, "grp": og}, device_id_type=MESH,
            ).start()
        recv[p, parity, pair] = send[p, me]

    loads[4].wait()
    gates = [
        jnp.broadcast_to(gates_ref[k : k + 1, :], (tok, tok)).T for k in range(2)
    ]
    loads[5].wait()
    loads[6].wait()
    step = 512
    for p in range(parts):
        pltpu.make_async_copy(whole(answer.at[p]), whole(answer.at[p]), dr.at[p]).wait()
        rows = (
            (recv[p, 0].astype(F32) + recv[p, 1].astype(F32)).reshape(2 * total, part).astype(BF)
        )
        for j in range(ff // step):
            here = slice(j * step, (j + 1) * step)
            term = jnp.dot(
                rows, up[p * part : (p + 1) * part, here], preferred_element_type=F32
            )
            if p > 0:
                term = partial[:, here] + term
            if p < parts - 1:
                partial[:, here] = term
            else:
                hidden[:, here] = jax.nn.gelu(term).astype(BF)

    step = 256
    for p in range(parts):
        for j in range(part // step):
            here = slice(j * step, (j + 1) * step)
            back[p, :, :, here] = (
                jnp.dot(
                    hidden[...], down[:, p * part + j * step : p * part + (j + 1) * step],
                    preferred_element_type=F32,
                )
                .reshape(total // 2, 4, step)
                .astype(BF)
            )
        for os, og in others:
            pltpu.make_async_remote_copy(
                src_ref=back.at[p, og * (seqs // 2) + os // 2], dst_ref=answer.at[p, me],
                send_sem=bs.at[p], recv_sem=br.at[p],
                device_id={"seq": os, "grp": og}, device_id_type=MESH,
            ).start()
        answer[p, me] = back[p, pair]

    for p in range(parts):
        pltpu.make_async_copy(whole(answer.at[p]), whole(answer.at[p]), ds.at[p]).wait()
    for p in range(parts):
        here = slice(p * part, (p + 1) * part)
        pltpu.make_async_copy(whole(answer.at[p]), whole(answer.at[p]), br.at[p]).wait()
        answers = answer[p].astype(F32).reshape(4 * total, part).astype(BF)
        mixed = residual[:, here]
        for k in range(2):
            picked = lax.dot_general(
                onehot[k], answers, (((0,), (0,)), ((), ())), preferred_element_type=F32
            )
            mixed = mixed + picked * jnp.concatenate([gates[k]] * (part // tok), axis=1)
        out_ref[:, here] = mixed.astype(BF)
    for p in range(parts):
        pltpu.make_async_copy(whole(answer.at[p]), whole(answer.at[p]), bs.at[p]).wait()


def experts(att, partner, routes, gates, states, gain, out_weight, up, down):
    tok, model = states.shape
    ff = up.shape[2]
    total = 128
    parts = 2
    part = model // parts
    hbm = pl.BlockSpec(memory_space=pltpu.HBM)
    vmem = pl.BlockSpec(memory_space=pltpu.VMEM)
    dma = pltpu.SemaphoreType.DMA
    return pl.pallas_call(
        experts_kernel,
        out_shape=jax.ShapeDtypeStruct((tok, model), BF),
        in_specs=[hbm] * 9,
        out_specs=vmem,
        scratch_shapes=[
            pltpu.VMEM((model, tok), BF),
            pltpu.VMEM((2, tok), jnp.int32),
            pltpu.VMEM((2, tok), jnp.int32),
            pltpu.VMEM((2, tok), F32),
            pltpu.VMEM((tok, model), BF),
            pltpu.VMEM((1, model), F32),
            pltpu.VMEM((model, model), BF),
            pltpu.VMEM((model, ff), BF),
            pltpu.VMEM((ff, model), BF),
            pltpu.VMEM((parts, total, 4, part), BF),
            pltpu.VMEM((parts, 2, total // 2, 4, part), BF),
            pltpu.VMEM((2 * total, ff), F32),
            pltpu.VMEM((2 * total, ff), BF),
            pltpu.VMEM((parts, total // 2, 4, part), BF),
            pltpu.VMEM((parts, total, 4, part), BF),
            dma((9,)),
        ]
        + [dma((parts,))] * 4,
        compiler_params=pltpu.CompilerParams(
            collective_id=1, has_side_effects=True, vmem_limit_bytes=VMEM_ALL
        ),
        name="experts",
    )(att, partner, routes, gates, states, gain, out_weight, up, down)


def body(
    queries, states, behavior_keys, behavior_values, lengths, user_of, out_weight, norm_gain,
    routes, route_weights, expert_up, expert_down,
):
    routes_t = routes.T
    att, partner = attention(
        queries, behavior_keys, behavior_values, lengths.reshape(1, -1), user_of.reshape(1, -1),
        routes_t,
    )
    return experts(
        att, partner, routes_t, route_weights.T, states, norm_gain.reshape(1, -1), out_weight,
        expert_up, expert_down,
    )


def solution(mesh):
    return jax.shard_map(
        body,
        mesh=mesh,
        in_specs=(
            P(("grp", "seq"), None),
            P(("grp", "seq"), None),
            P("grp", "seq", None),
            P("grp", "seq", None),
            P("grp"),
            P("grp"),
            P(),
            P(),
            P(("grp", "seq"), None),
            P(("grp", "seq"), None),
            P(("seq", "grp"), None, None),
            P(("seq", "grp"), None, None),
        ),
        out_specs=P(("grp", "seq"), None),
        check_vma=False,
    )
```

```python
import itertools
import math

import jax
import jax.numpy as jnp
from jax import lax
from jax.experimental import pallas as pl
from jax.experimental.pallas import tpu as pltpu
from jax.sharding import PartitionSpec as P

HEADS = 8
MESH = pl.DeviceIdType.MESH
BF = jnp.bfloat16
F32 = jnp.float32
LOW = -1e30
VMEM_ALL = 67043328
SEQS = 16
GRPS = 8

FULL = ((0, 1), (0, 3), (1, 0), (3, 0))
FIRST = ((1, 1), (1, 3), (2, 0))
SECOND = ((3, 3), (3, 1), (0, 2))
HALVES = FIRST + SECOND


def head_of(y, z):
    return (y % 2) * 4 + (z + 2 * (y // 2)) % 4


def seq_of(y, z):
    return ((y + 8) % 4) * 4 + (z + 8) % 4


def far_first(steps):
    def hops(step):
        return sum(min(d, 4 - d) for d in step[:3])

    return sorted((s for s in steps if any(s)), key=lambda s: (-hops(s), sum(s) % 3, s))


def cols(head, width=128):
    return pl.ds(pl.multiple_of(head * width, width), width)


def block_kernel(
    q_hbm, k_hbm, v_hbm, len_hbm, user_hbm, routes_hbm, gates_hbm, states_hbm, gain_hbm,
    wo_hbm, up_hbm, down_hbm,
    out_ref,
    len_ref, user_ref, routes_ref, q_v, k_v, v_v, qbuf, kcat, vcat, qt, vt, score, prob, acc,
    osend, obuf, ssend, sbuf, rbuf,
    gates_ref, states_ref, gain_ref, wo, up, down,
    onehot, gate, att, residual, send, recv, partial, hidden, back, answer,
    load_sem, own_sem, qs, qr, ks, kr, vs, vr, os, orr, ss, sr, rs, rr, ds, dr, bs, br, ready,
):
    me, g = lax.axis_index("seq"), lax.axis_index("grp")
    y, z = me // 4, me % 4
    head = head_of(y, z)
    hist = k_hbm.shape[1]
    half = hist // 2
    tok, model = q_hbm.shape
    ff = up.shape[1]
    width = model // HEADS
    scale = math.log2(math.e) / math.sqrt(width)
    total = SEQS * GRPS
    mine = me * GRPS + g
    parity = me % 2
    pair = g * (SEQS // 2) + me // 2
    parts = send.shape[0]
    part = model // parts

    def load(i, src, dst):
        return pltpu.make_async_copy(src, dst, load_sem.at[i])

    loads = [
        load(0, q_hbm, q_v), load(1, k_hbm, k_v), load(2, v_hbm, v_v),
        load(3, routes_hbm, routes_ref), load(4, user_hbm, user_ref), load(5, len_hbm, len_ref),
        load(6, wo_hbm, wo), load(7, states_hbm, states_ref), load(8, gain_hbm, gain_ref),
        load(9, gates_hbm, gates_ref), load(10, up_hbm.at[0], up), load(11, down_hbm.at[0], down),
    ]
    for copy in loads[:6]:
        copy.start()
    own = [pltpu.make_async_copy(q_hbm.at[:, cols(head)], qbuf.at[me], own_sem.at[0])]
    for i, (src, dst) in enumerate(((k_hbm, kcat), (v_hbm, vcat))):
        for user in range(2):
            own.append(
                pltpu.make_async_copy(
                    src.at[user, :, cols(head)],
                    dst.at[pl.ds(0, hist), pl.ds(user * width, width)],
                    own_sem.at[1 + 2 * i + user],
                )
            )
    for copy in own:
        copy.start()

    barrier = pltpu.get_barrier_semaphore()
    seq_peers = [
        seq_of(y + dy, z + dz) for dy, dz in far_first(itertools.product(range(4), range(4)))
    ]
    for other in seq_peers:
        pl.semaphore_signal(barrier, inc=1, device_id={"seq": other}, device_id_type=MESH)
    for step in range(1, GRPS):
        pl.semaphore_signal(
            barrier, inc=1, device_id={"grp": (g + step) % GRPS}, device_id_type=MESH
        )
    pl.semaphore_wait(barrier, SEQS - 1 + GRPS - 1)

    loads[0].wait()
    for dy, dz in far_first(itertools.product(range(4), range(4))):
        ty, tz = (y + dy) % 4, (z + dz) % 4
        pltpu.make_async_remote_copy(
            src_ref=q_v.at[:, cols(head_of(ty, tz))],
            dst_ref=qbuf.at[me],
            send_sem=qs, recv_sem=qr,
            device_id={"seq": ty * 4 + tz}, device_id_type=MESH,
        ).start()

    def send_halves(src, dst, send_sem, recv_sem):
        for j, (dy, dz) in enumerate(HALVES):
            ty, tz = (y - dy + 4) % 4, (z - dz + 4) % 4
            first = 0 if (dy, dz) in FIRST else half
            for user in range(2):
                pltpu.make_async_remote_copy(
                    src_ref=src.at[user, pl.ds(first, half), cols(head_of(ty, tz))],
                    dst_ref=dst.at[pl.ds(5 * hist + j * half, half), pl.ds(user * width, width)],
                    send_sem=send_sem, recv_sem=recv_sem,
                    device_id={"seq": ty * 4 + tz}, device_id_type=MESH,
                ).start()

    def send_fulls(src, dst, send_sem, recv_sem):
        for j, (dy, dz) in enumerate(FULL):
            ty, tz = (y - dy + 4) % 4, (z - dz + 4) % 4
            for user in range(2):
                pltpu.make_async_remote_copy(
                    src_ref=src.at[user, :, cols(head_of(ty, tz))],
                    dst_ref=dst.at[pl.ds((1 + j) * hist, hist), pl.ds(user * width, width)],
                    send_sem=send_sem, recv_sem=recv_sem,
                    device_id={"seq": ty * 4 + tz}, device_id_type=MESH,
                ).start()

    loads[1].wait()
    send_halves(k_v, kcat, ks, kr)
    send_fulls(k_v, kcat, ks, kr)
    loads[2].wait()
    send_halves(v_v, vcat, vs.at[0], vr.at[0])
    send_fulls(v_v, vcat, vs.at[1], vr.at[1])

    partner = me + 1 - 2 * parity
    loads[3].wait()
    route_copy = pltpu.make_async_remote_copy(
        src_ref=routes_ref, dst_ref=rbuf, send_sem=rs, recv_sem=rr,
        device_id={"seq": partner}, device_id_type=MESH,
    )
    route_copy.start()
    for other in seq_peers:
        pl.semaphore_signal(ready, inc=1, device_id={"seq": other}, device_id_type=MESH)
    for copy in loads[6:]:
        copy.start()

    starts = []
    for dy, dz in ((0, 0),) + FULL:
        base = seq_of(y + dy, z + dz) * hist
        starts += [base, base + half]
    for dy, dz in HALVES:
        base = seq_of(y + dy, z + dz) * hist
        starts.append(base if (dy, dz) in FIRST else base + half)

    loads[4].wait()
    loads[5].wait()
    own[0].wait()
    moved = pl.ds(0, SEQS - 1)
    pltpu.make_async_copy(qbuf.at[moved], qbuf.at[moved], qr).wait()
    for i in range(SEQS):
        flipped = qbuf[i].T
        users = user_ref[:, i * tok : (i + 1) * tok]
        for user in range(2):
            qt[user * width : (user + 1) * width, i * tok : (i + 1) * tok] = jnp.where(
                users == user, flipped, jnp.zeros_like(flipped)
            )

    route_copy.wait()
    experts = lax.broadcasted_iota(jnp.int32, (total, tok), 0)
    named = [(routes_ref[k : k + 1, :] == experts).astype(F32) for k in range(2)]
    theirs = sum((rbuf[k : k + 1, :] == experts).astype(F32) for k in range(2))
    earlier = (
        lax.broadcasted_iota(jnp.int32, (tok, tok), 0) < lax.broadcasted_iota(jnp.int32, (tok, tok), 1)
    ).astype(BF)
    rank = jnp.dot((named[0] + named[1]).astype(BF), earlier, preferred_element_type=F32)
    ahead = jnp.dot(theirs.astype(BF), jnp.ones((tok, tok), BF), preferred_element_type=F32)
    rank = rank + ahead * parity.astype(F32)
    places = lax.broadcasted_iota(jnp.int32, (4 * total, tok), 0)
    loads[9].wait()
    for k in range(2):
        slot = jnp.sum(named[k] * rank, axis=0, keepdims=True).astype(jnp.int32)
        target = routes_ref[k : k + 1, :] * 4 + slot
        onehot[k] = (places == target).astype(F32).astype(BF)
        gate[k] = jnp.broadcast_to(gates_ref[k : k + 1, :], (tok, tok)).T

    own[1].wait()
    own[2].wait()
    far = pl.ds(5 * hist, 6 * half)
    near = pl.ds(hist, 4 * hist)
    rest = pl.ds(hist, kcat.shape[0] - hist)
    pltpu.make_async_copy(kcat.at[rest], kcat.at[rest], kr).wait()

    block = 4 * tok
    rows_y = [(y + dy) % 4 for dy in (2, 1, 3, 0)]
    limit0 = len_ref[0:1, 0:1]
    limit1 = len_ref[0:1, 1:2]

    def tokens_of(row):
        return pl.ds(pl.multiple_of(row * block, block), block)

    stat = []
    for row in rows_y:
        here = tokens_of(row)
        limit = jnp.where(user_ref[:, here] == 0, limit0, limit1)
        top = jnp.full((8, block), LOW, F32)
        for c, start in enumerate(starts):
            s = jnp.dot(kcat[c * half : (c + 1) * half, :], qt[:, here], preferred_element_type=F32)
            pos = start + lax.broadcasted_iota(jnp.int32, (half, block), 0)
            s = jnp.where(pos < limit, s, LOW)
            score[c * half : (c + 1) * half, :] = s
            top = jnp.maximum(top, s.reshape(half // 8, 8, block).max(0))
        peak = top.max(0, keepdims=True)
        denom = jnp.zeros((8, block), F32)
        for c in range(len(starts)):
            p = jnp.exp2((score[c * half : (c + 1) * half, :] - peak) * scale)
            denom = denom + p.reshape(half // 8, 8, block).sum(0)
            prob[c * half : (c + 1) * half, here] = p.astype(BF)
        stat.append((peak, denom.sum(0, keepdims=True)))

    own[3].wait()
    own[4].wait()
    pltpu.make_async_copy(vcat.at[far], vcat.at[far], vr.at[0]).wait()
    split = 5 * hist
    vt[:, split:] = vcat[split:, :].T
    for row in rows_y:
        here = tokens_of(row)
        acc[:, here] = jnp.dot(vt[:, split:], prob[split:, here], preferred_element_type=F32)
    pltpu.make_async_copy(vcat.at[near], vcat.at[near], vr.at[1]).wait()
    vt[:, :split] = vcat[:split, :].T

    for row, (peak, denom) in zip(rows_y, stat):
        here = tokens_of(row)
        both = acc[:, here] + jnp.dot(vt[:, :split], prob[:split, here], preferred_element_type=F32)
        out = jnp.where(user_ref[:, here] == 0, both[:width], both[width:]) * (1.0 / denom)
        out = out.astype(BF)
        packed = jnp.concatenate([peak, denom, jnp.zeros((6, block), F32)], axis=0)
        for i in range(4):
            osend[row * 4 + i] = out[:, i * tok : (i + 1) * tok]
            ssend[row * 4 + i] = packed[:, i * tok : (i + 1) * tok]
        for dz in (2, 1, 3, 0):
            owner = row * 4 + (z + dz) % 4
            if dz == 0 and row is rows_y[-1]:
                continue
            pltpu.make_async_remote_copy(
                src_ref=osend.at[owner], dst_ref=obuf.at[me], send_sem=os, recv_sem=orr,
                device_id={"seq": owner}, device_id_type=MESH,
            ).start()
            pltpu.make_async_remote_copy(
                src_ref=ssend.at[owner], dst_ref=sbuf.at[me], send_sem=ss, recv_sem=sr,
                device_id={"seq": owner}, device_id_type=MESH,
            ).start()

    obuf[me] = osend[me]
    sbuf[me] = ssend[me]
    pltpu.make_async_copy(qbuf.at[moved], qbuf.at[moved], qs).wait()
    pltpu.make_async_copy(kcat.at[rest], kcat.at[rest], ks).wait()
    pltpu.make_async_copy(vcat.at[far], vcat.at[far], vs.at[0]).wait()
    pltpu.make_async_copy(vcat.at[near], vcat.at[near], vs.at[1]).wait()
    for i in (6, 7, 8):
        loads[i].wait()

    ys = [(y + d) % 4 * 4 for d in range(4)]
    zs = [(z + d) % 4 for d in range(4)]
    xs = [(g // 2 + d) % 4 * 2 for d in range(4)]
    cs = [(g + d) % 2 for d in range(2)]
    others = [
        (ys[dy] + zs[dz], xs[dx] + cs[dc])
        for dy, dz, dx, dc in far_first(itertools.product(range(4), range(4), range(4), range(2)))
    ]
    pl.semaphore_wait(ready, SEQS - 1)

    pltpu.make_async_copy(sbuf.at[moved], sbuf.at[moved], sr).wait()
    pltpu.make_async_copy(obuf.at[moved], obuf.at[moved], orr).wait()
    for h in range(HEADS):
        hy, hz = h // 4, h % 4
        first = hy * 4 + hz
        second = (hy + 2) * 4 + (hz + 2) % 4
        m0, d0 = sbuf[first, 0:1], sbuf[first, 1:2]
        m1, d1 = sbuf[second, 0:1], sbuf[second, 1:2]
        top = jnp.maximum(m0, m1)
        w0 = d0 * jnp.exp2((m0 - top) * scale)
        w1 = d1 * jnp.exp2((m1 - top) * scale)
        inverse = 1.0 / (w0 + w1)
        merged = obuf[first].astype(F32) * (w0 * inverse) + obuf[second].astype(F32) * (w1 * inverse)
        att[h * width : (h + 1) * width, :] = merged.astype(BF)

    res = states_ref[...].astype(F32) + lax.dot_general(
        att[...], wo[...], (((0,), (0,)), ((), ())), preferred_element_type=F32
    )
    residual[...] = res
    spread = jnp.mean(res * res, axis=-1, keepdims=True)
    normed = (res / jnp.sqrt(spread + 1e-06) * gain_ref[...]).astype(BF)
    placed = onehot[0] + onehot[1]

    def whole(buffer):
        return buffer.at[pl.ds(0, total - 1)]

    for p in range(parts):
        send[p] = (
            jnp.dot(placed, normed[:, p * part : (p + 1) * part], preferred_element_type=F32)
            .reshape(total, 4, part)
            .astype(BF)
        )
        for other, og in others:
            pltpu.make_async_remote_copy(
                src_ref=send.at[p, other * GRPS + og], dst_ref=recv.at[p, parity, pair],
                send_sem=ds.at[p], recv_sem=dr.at[p],
                device_id={"seq": other, "grp": og}, device_id_type=MESH,
            ).start()
        recv[p, parity, pair] = send[p, mine]

    pltpu.make_async_copy(obuf.at[moved], obuf.at[moved], os).wait()
    pltpu.make_async_copy(sbuf.at[moved], sbuf.at[moved], ss).wait()
    loads[10].wait()
    loads[11].wait()
    step = 512
    for p in range(parts):
        pltpu.make_async_copy(whole(answer.at[p]), whole(answer.at[p]), dr.at[p]).wait()
        rows = (
            (recv[p, 0].astype(F32) + recv[p, 1].astype(F32)).reshape(2 * total, part).astype(BF)
        )
        for j in range(ff // step):
            here = slice(j * step, (j + 1) * step)
            term = jnp.dot(
                rows, up[p * part : (p + 1) * part, here], preferred_element_type=F32
            )
            if p > 0:
                term = partial[:, here] + term
            if p < parts - 1:
                partial[:, here] = term
            else:
                hidden[:, here] = jax.nn.gelu(term).astype(BF)

    step = 256
    for p in range(parts):
        for j in range(part // step):
            here = slice(j * step, (j + 1) * step)
            back[p, :, :, here] = (
                jnp.dot(
                    hidden[...], down[:, p * part + j * step : p * part + (j + 1) * step],
                    preferred_element_type=F32,
                )
                .reshape(total // 2, 4, step)
                .astype(BF)
            )
        for other, og in others:
            pltpu.make_async_remote_copy(
                src_ref=back.at[p, og * (SEQS // 2) + other // 2], dst_ref=answer.at[p, mine],
                send_sem=bs.at[p], recv_sem=br.at[p],
                device_id={"seq": other, "grp": og}, device_id_type=MESH,
            ).start()
        answer[p, mine] = back[p, pair]

    for p in range(parts):
        pltpu.make_async_copy(whole(answer.at[p]), whole(answer.at[p]), ds.at[p]).wait()
    for p in range(parts):
        here = slice(p * part, (p + 1) * part)
        pltpu.make_async_copy(whole(answer.at[p]), whole(answer.at[p]), br.at[p]).wait()
        answers = answer[p].astype(F32).reshape(4 * total, part).astype(BF)
        mixed = residual[:, here]
        for k in range(2):
            picked = lax.dot_general(
                onehot[k], answers, (((0,), (0,)), ((), ())), preferred_element_type=F32
            )
            mixed = mixed + picked * jnp.concatenate([gate[k]] * (part // tok), axis=1)
        out_ref[:, here] = mixed.astype(BF)
    for p in range(parts):
        pltpu.make_async_copy(whole(answer.at[p]), whole(answer.at[p]), bs.at[p]).wait()


def body(
    queries, states, behavior_keys, behavior_values, lengths, user_of, out_weight, norm_gain,
    routes, route_weights, expert_up, expert_down,
):
    tok, model = queries.shape
    hist = behavior_keys.shape[1]
    ff = expert_up.shape[2]
    width = model // HEADS
    held = 8 * hist
    total = SEQS * GRPS
    parts = 2
    part = model // parts
    hbm = pl.BlockSpec(memory_space=pltpu.HBM)
    vmem = pltpu.VMEM
    dma = pltpu.SemaphoreType.DMA
    return pl.pallas_call(
        block_kernel,
        out_shape=jax.ShapeDtypeStruct((tok, model), BF),
        in_specs=[hbm] * 12,
        out_specs=pl.BlockSpec(memory_space=vmem),
        scratch_shapes=[
            vmem((1, 2), jnp.int32),
            vmem((1, SEQS * tok), jnp.int32),
            vmem((2, tok), jnp.int32),
            vmem((tok, model), BF),
            vmem((2, hist, model), BF),
            vmem((2, hist, model), BF),
            vmem((SEQS, tok, width), BF),
            vmem((held, 2 * width), BF),
            vmem((held, 2 * width), BF),
            vmem((2 * width, SEQS * tok), BF),
            vmem((2 * width, held), BF),
            vmem((held, 4 * tok), F32),
            vmem((held, SEQS * tok), BF),
            vmem((2 * width, SEQS * tok), F32),
            vmem((SEQS, width, tok), BF),
            vmem((SEQS, width, tok), BF),
            vmem((SEQS, 8, tok), F32),
            vmem((SEQS, 8, tok), F32),
            vmem((2, tok), jnp.int32),
            vmem((2, tok), F32),
            vmem((tok, model), BF),
            vmem((1, model), F32),
            vmem((model, model), BF),
            vmem((model, ff), BF),
            vmem((ff, model), BF),
            vmem((2, 4 * total, tok), BF),
            vmem((2, tok, tok), F32),
            vmem((model, tok), BF),
            vmem((tok, model), F32),
            vmem((parts, total, 4, part), BF),
            vmem((parts, 2, total // 2, 4, part), BF),
            vmem((2 * total, ff), F32),
            vmem((2 * total, ff), BF),
            vmem((parts, total // 2, 4, part), BF),
            vmem((parts, total, 4, part), BF),
            dma((12,)),
            dma((5,)),
            dma, dma, dma, dma,
            dma((2,)),
            dma((2,)),
            dma, dma, dma, dma, dma, dma,
        ]
        + [dma((parts,))] * 4
        + [pltpu.SemaphoreType.REGULAR],
        compiler_params=pltpu.CompilerParams(
            collective_id=0, has_side_effects=True, vmem_limit_bytes=VMEM_ALL
        ),
        name="decoder_block",
    )(
        queries, behavior_keys, behavior_values, lengths.reshape(1, -1), user_of.reshape(1, -1),
        routes.T, route_weights.T, states, norm_gain.reshape(1, -1), out_weight, expert_up,
        expert_down,
    )


def solution(mesh):
    return jax.shard_map(
        body,
        mesh=mesh,
        in_specs=(
            P(("grp", "seq"), None),
            P(("grp", "seq"), None),
            P("grp", "seq", None),
            P("grp", "seq", None),
            P("grp"),
            P("grp"),
            P(),
            P(),
            P(("grp", "seq"), None),
            P(("grp", "seq"), None),
            P(("seq", "grp"), None, None),
            P(("seq", "grp"), None, None),
        ),
        out_specs=P(("grp", "seq"), None),
        check_vma=False,
    )
```

```python
import itertools
import math

import jax
import jax.numpy as jnp
from jax import lax
from jax.experimental import pallas as pl
from jax.experimental.pallas import tpu as pltpu
from jax.sharding import PartitionSpec as P

HEADS = 8
MESH = pl.DeviceIdType.MESH
BF = jnp.bfloat16
F32 = jnp.float32
LOW = -1e30
VMEM_ALL = 67043328
SEQS = 16
GRPS = 8

FULL = ((0, 1), (0, 3), (1, 0), (3, 0))
FIRST = ((1, 1), (1, 3), (2, 0))
SECOND = ((3, 3), (3, 1), (0, 2))
HALVES = FIRST + SECOND

GROUPS = (
    ((2, 2), (1, 1), (3, 3), (2, 0), (0, 2), (1, 3), (3, 1), (0, 0)),
    ((1, 2), (2, 3), (3, 2), (2, 1), (1, 0), (0, 3), (3, 0), (0, 1)),
)


def head_of(y, z):
    return (y % 2) * 4 + (z + 2 * (y // 2)) % 4


def seq_of(y, z):
    return ((y + 8) % 4) * 4 + (z + 8) % 4


def far_first(steps):
    def hops(step):
        return sum(min(d, 4 - d) for d in step[:3])

    return sorted((s for s in steps if any(s)), key=lambda s: (-hops(s), sum(s) % 3, s))


def cols(head, width=128):
    return pl.ds(pl.multiple_of(head * width, width), width)


def block_kernel(
    q_hbm, k_hbm, v_hbm, len_hbm, user_hbm, routes_hbm, gates_hbm, states_hbm, gain_hbm,
    wo_hbm, up_hbm, down_hbm,
    out_ref,
    len_ref, user_ref, routes_ref, q_v, k_v, v_v, qbuf, kcat, vcat, qt, vt, score, prob, acc,
    osend, obuf, ssend, sbuf, rbuf,
    gates_ref, states_ref, gain_ref, wo, up, down,
    onehot, gate, att, residual, send, recv, hidden, back, answer,
    load_sem, own_sem, qs, qr, ks, kr, vs, vr, os, orr, ss, sr, rs, rr, ds, dr, bs, br, ready,
):
    me, g = lax.axis_index("seq"), lax.axis_index("grp")
    y, z = me // 4, me % 4
    head = head_of(y, z)
    hist = k_hbm.shape[1]
    half = hist // 2
    tok, model = q_hbm.shape
    ff = up.shape[1]
    width = model // HEADS
    scale = math.log2(math.e) / math.sqrt(width)
    total = SEQS * GRPS
    mine = me * GRPS + g
    parity = me % 2

    def load(i, src, dst):
        return pltpu.make_async_copy(src, dst, load_sem.at[i])

    loads = [
        load(0, q_hbm, q_v), load(1, k_hbm, k_v), load(2, v_hbm, v_v),
        load(3, routes_hbm, routes_ref), load(4, user_hbm, user_ref), load(5, len_hbm, len_ref),
        load(6, wo_hbm, wo), load(7, states_hbm, states_ref), load(8, gain_hbm, gain_ref),
        load(9, gates_hbm, gates_ref), load(10, up_hbm.at[0], up), load(11, down_hbm.at[0], down),
    ]
    for copy in loads[:6]:
        copy.start()
    own = [pltpu.make_async_copy(q_hbm.at[:, cols(head)], qbuf.at[me], own_sem.at[0])]
    for i, (src, dst) in enumerate(((k_hbm, kcat), (v_hbm, vcat))):
        for user in range(2):
            own.append(
                pltpu.make_async_copy(
                    src.at[user, :, cols(head)],
                    dst.at[pl.ds(0, hist), pl.ds(user * width, width)],
                    own_sem.at[1 + 2 * i + user],
                )
            )
    for copy in own:
        copy.start()

    barrier = pltpu.get_barrier_semaphore()
    seq_peers = [
        seq_of(y + dy, z + dz) for dy, dz in far_first(itertools.product(range(4), range(4)))
    ]
    for other in seq_peers:
        pl.semaphore_signal(barrier, inc=1, device_id={"seq": other}, device_id_type=MESH)
    for step in range(1, GRPS):
        pl.semaphore_signal(
            barrier, inc=1, device_id={"grp": (g + step) % GRPS}, device_id_type=MESH
        )
    pl.semaphore_wait(barrier, SEQS - 1 + GRPS - 1)

    partner = me + 1 - 2 * parity
    loads[3].wait()
    route_copy = pltpu.make_async_remote_copy(
        src_ref=routes_ref, dst_ref=rbuf, send_sem=rs, recv_sem=rr,
        device_id={"seq": partner}, device_id_type=MESH,
    )
    route_copy.start()
    loads[0].wait()
    for dy, dz in far_first(itertools.product(range(4), range(4))):
        ty, tz = (y + dy) % 4, (z + dz) % 4
        pltpu.make_async_remote_copy(
            src_ref=q_v.at[:, cols(head_of(ty, tz))],
            dst_ref=qbuf.at[me],
            send_sem=qs, recv_sem=qr,
            device_id={"seq": ty * 4 + tz}, device_id_type=MESH,
        ).start()

    def send_halves(src, dst, send_sem, recv_sem):
        for j, (dy, dz) in enumerate(HALVES):
            ty, tz = (y - dy + 4) % 4, (z - dz + 4) % 4
            first = 0 if (dy, dz) in FIRST else half
            for user in range(2):
                pltpu.make_async_remote_copy(
                    src_ref=src.at[user, pl.ds(first, half), cols(head_of(ty, tz))],
                    dst_ref=dst.at[pl.ds(5 * hist + j * half, half), pl.ds(user * width, width)],
                    send_sem=send_sem, recv_sem=recv_sem,
                    device_id={"seq": ty * 4 + tz}, device_id_type=MESH,
                ).start()

    def send_fulls(src, dst, send_sem, recv_sem):
        for j, (dy, dz) in enumerate(FULL):
            ty, tz = (y - dy + 4) % 4, (z - dz + 4) % 4
            for user in range(2):
                pltpu.make_async_remote_copy(
                    src_ref=src.at[user, :, cols(head_of(ty, tz))],
                    dst_ref=dst.at[pl.ds((1 + j) * hist, hist), pl.ds(user * width, width)],
                    send_sem=send_sem, recv_sem=recv_sem,
                    device_id={"seq": ty * 4 + tz}, device_id_type=MESH,
                ).start()

    loads[1].wait()
    send_halves(k_v, kcat, ks, kr)
    send_fulls(k_v, kcat, ks, kr)
    loads[2].wait()
    send_halves(v_v, vcat, vs.at[0], vr.at[0])
    send_fulls(v_v, vcat, vs.at[1], vr.at[1])

    for other in seq_peers:
        pl.semaphore_signal(ready, inc=1, device_id={"seq": other}, device_id_type=MESH)
    for copy in loads[6:]:
        copy.start()

    starts = []
    for dy, dz in ((0, 0),) + FULL:
        base = seq_of(y + dy, z + dz) * hist
        starts += [base, base + half]
    for dy, dz in HALVES:
        base = seq_of(y + dy, z + dz) * hist
        starts.append(base if (dy, dz) in FIRST else base + half)

    loads[4].wait()
    loads[5].wait()
    own[0].wait()
    moved = pl.ds(0, SEQS - 1)
    pltpu.make_async_copy(qbuf.at[moved], qbuf.at[moved], qr).wait()
    for i in range(SEQS):
        flipped = qbuf[i].T
        users = user_ref[:, i * tok : (i + 1) * tok]
        for user in range(2):
            qt[user * width : (user + 1) * width, i * tok : (i + 1) * tok] = jnp.where(
                users == user, flipped, jnp.zeros_like(flipped)
            )

    route_copy.wait()
    experts = lax.broadcasted_iota(jnp.int32, (total, tok), 0)
    named = [(routes_ref[k : k + 1, :] == experts).astype(F32) for k in range(2)]
    theirs = sum((rbuf[k : k + 1, :] == experts).astype(F32) for k in range(2))
    earlier = (
        lax.broadcasted_iota(jnp.int32, (tok, tok), 0) < lax.broadcasted_iota(jnp.int32, (tok, tok), 1)
    ).astype(BF)
    rank = jnp.dot((named[0] + named[1]).astype(BF), earlier, preferred_element_type=F32)
    ahead = jnp.dot(theirs.astype(BF), jnp.ones((tok, tok), BF), preferred_element_type=F32)
    rank = rank + ahead * parity.astype(F32)
    places = lax.broadcasted_iota(jnp.int32, (4 * total, tok), 0)
    loads[9].wait()
    for k in range(2):
        slot = jnp.sum(named[k] * rank, axis=0, keepdims=True).astype(jnp.int32)
        target = routes_ref[k : k + 1, :] * 4 + slot
        onehot[k] = (places == target).astype(F32).astype(BF)
        gate[k] = jnp.broadcast_to(gates_ref[k : k + 1, :], (tok, tok)).T

    own[1].wait()
    own[2].wait()
    far = pl.ds(5 * hist, 6 * half)
    near = pl.ds(hist, 4 * hist)
    rest = pl.ds(hist, kcat.shape[0] - hist)
    pltpu.make_async_copy(kcat.at[rest], kcat.at[rest], kr).wait()

    block = 4 * tok
    rows_y = [(y + dy) % 4 for dy in (2, 1, 3, 0)]
    limit0 = len_ref[0:1, 0:1]
    limit1 = len_ref[0:1, 1:2]

    def tokens_of(row):
        return pl.ds(pl.multiple_of(row * block, block), block)

    stat = []
    for row in rows_y:
        here = tokens_of(row)
        limit = jnp.where(user_ref[:, here] == 0, limit0, limit1)
        top = jnp.full((8, block), LOW, F32)
        for c, start in enumerate(starts):
            s = jnp.dot(kcat[c * half : (c + 1) * half, :], qt[:, here], preferred_element_type=F32)
            pos = start + lax.broadcasted_iota(jnp.int32, (half, block), 0)
            s = jnp.where(pos < limit, s, LOW)
            score[c * half : (c + 1) * half, :] = s
            top = jnp.maximum(top, s.reshape(half // 8, 8, block).max(0))
        peak = top.max(0, keepdims=True)
        denom = jnp.zeros((8, block), F32)
        for c in range(len(starts)):
            p = jnp.exp2((score[c * half : (c + 1) * half, :] - peak) * scale)
            denom = denom + p.reshape(half // 8, 8, block).sum(0)
            prob[c * half : (c + 1) * half, here] = p.astype(BF)
        stat.append((peak, denom.sum(0, keepdims=True)))

    own[3].wait()
    own[4].wait()
    pltpu.make_async_copy(vcat.at[far], vcat.at[far], vr.at[0]).wait()
    split = 5 * hist
    vt[:, split:] = vcat[split:, :].T
    for row in rows_y:
        here = tokens_of(row)
        acc[:, here] = jnp.dot(vt[:, split:], prob[split:, here], preferred_element_type=F32)
    pltpu.make_async_copy(vcat.at[near], vcat.at[near], vr.at[1]).wait()
    vt[:, :split] = vcat[:split, :].T

    for row, (peak, denom) in zip(rows_y, stat):
        here = tokens_of(row)
        both = acc[:, here] + jnp.dot(vt[:, :split], prob[:split, here], preferred_element_type=F32)
        out = jnp.where(user_ref[:, here] == 0, both[:width], both[width:]) * (1.0 / denom)
        out = out.astype(BF)
        packed = jnp.concatenate([peak, denom, jnp.zeros((6, block), F32)], axis=0)
        for i in range(4):
            osend[row * 4 + i] = out[:, i * tok : (i + 1) * tok]
            ssend[row * 4 + i] = packed[:, i * tok : (i + 1) * tok]
        for dz in (2, 1, 3, 0):
            owner = row * 4 + (z + dz) % 4
            if dz == 0 and row is rows_y[-1]:
                continue
            pltpu.make_async_remote_copy(
                src_ref=osend.at[owner], dst_ref=obuf.at[me], send_sem=os, recv_sem=orr,
                device_id={"seq": owner}, device_id_type=MESH,
            ).start()
            pltpu.make_async_remote_copy(
                src_ref=ssend.at[owner], dst_ref=sbuf.at[me], send_sem=ss, recv_sem=sr,
                device_id={"seq": owner}, device_id_type=MESH,
            ).start()

    obuf[me] = osend[me]
    sbuf[me] = ssend[me]
    pltpu.make_async_copy(qbuf.at[moved], qbuf.at[moved], qs).wait()
    pltpu.make_async_copy(kcat.at[rest], kcat.at[rest], ks).wait()
    pltpu.make_async_copy(vcat.at[far], vcat.at[far], vs.at[0]).wait()
    pltpu.make_async_copy(vcat.at[near], vcat.at[near], vs.at[1]).wait()
    for i in (6, 7, 8):
        loads[i].wait()

    pl.semaphore_wait(ready, SEQS - 1)

    pltpu.make_async_copy(sbuf.at[moved], sbuf.at[moved], sr).wait()
    pltpu.make_async_copy(obuf.at[moved], obuf.at[moved], orr).wait()
    for h in range(HEADS):
        hy, hz = h // 4, h % 4
        first = hy * 4 + hz
        second = (hy + 2) * 4 + (hz + 2) % 4
        m0, d0 = sbuf[first, 0:1], sbuf[first, 1:2]
        m1, d1 = sbuf[second, 0:1], sbuf[second, 1:2]
        top = jnp.maximum(m0, m1)
        w0 = d0 * jnp.exp2((m0 - top) * scale)
        w1 = d1 * jnp.exp2((m1 - top) * scale)
        inverse = 1.0 / (w0 + w1)
        merged = obuf[first].astype(F32) * (w0 * inverse) + obuf[second].astype(F32) * (w1 * inverse)
        att[h * width : (h + 1) * width, :] = merged.astype(BF)

    res = states_ref[...].astype(F32) + lax.dot_general(
        att[...], wo[...], (((0,), (0,)), ((), ())), preferred_element_type=F32
    )
    residual[...] = res
    spread = jnp.mean(res * res, axis=-1, keepdims=True)
    normed = (res / jnp.sqrt(spread + 1e-06) * gain_ref[...]).astype(BF)
    placed = onehot[0] + onehot[1]

    zh, x, core = z // 2, g // 2, g % 2
    slots = list(itertools.product(range(8), range(2), range(2)))

    send[...] = (
        jnp.dot(placed, normed, preferred_element_type=F32).reshape(total, 4, model).astype(BF)
    )
    for n, steps in enumerate(GROUPS):
        for k, hz, hc in slots:
            dy, dx = steps[k]
            for low in range(2):
                other = (y - dy + 4) % 4 * 4 + (zh + hz) % 2 * 2 + low
                og = (x - dx + 4) % 4 * 2 + (core + hc) % 2
                slot = k * 4 + hz * 2 + hc

                def start(other=other, og=og, slot=slot, n=n):
                    pltpu.make_async_remote_copy(
                        src_ref=send.at[other * GRPS + og], dst_ref=recv.at[n, parity, slot],
                        send_sem=ds.at[n], recv_sem=dr.at[n],
                        device_id={"seq": other, "grp": og}, device_id_type=MESH,
                    ).start()

                if (dy, dx, hz, hc) == (0, 0, 0, 0):
                    pl.when(parity != low)(start)
                else:
                    start()
        if n == 0:
            pltpu.make_async_copy(answer.at[pl.ds(0, 63)], answer.at[pl.ds(0, 63)], ds.at[0]).wait()
    recv[0, parity, 28] = send[mine]

    pltpu.make_async_copy(obuf.at[moved], obuf.at[moved], os).wait()
    pltpu.make_async_copy(sbuf.at[moved], sbuf.at[moved], ss).wait()
    loads[10].wait()
    loads[11].wait()
    for n, steps in enumerate(GROUPS):
        come = pl.ds(0, 63 + n)
        pltpu.make_async_copy(answer.at[come], answer.at[come], dr.at[n]).wait()
        rows = (recv[n, 0].astype(F32) + recv[n, 1].astype(F32)).reshape(total, model).astype(BF)
        step = 512
        for j in range(ff // step):
            here = slice(j * step, (j + 1) * step)
            hidden[:, here] = jax.nn.gelu(
                jnp.dot(rows, up[:, here], preferred_element_type=F32)
            ).astype(BF)
        step = 256
        for j in range(model // step):
            here = slice(j * step, (j + 1) * step)
            back[n, :, :, here] = (
                jnp.dot(hidden[...], down[:, here], preferred_element_type=F32)
                .reshape(total // 4, 4, step)
                .astype(BF)
            )
        for k, hz, hc in slots:
            dy, dx = steps[k]
            for low in range(2):
                other = (y + dy) % 4 * 4 + (zh + hz) % 2 * 2 + low
                og = (x + dx) % 4 * 2 + (core + hc) % 2
                slot = k * 4 + hz * 2 + hc

                def start(other=other, og=og, slot=slot, n=n):
                    pltpu.make_async_remote_copy(
                        src_ref=back.at[n, slot], dst_ref=answer.at[mine],
                        send_sem=bs, recv_sem=br,
                        device_id={"seq": other, "grp": og}, device_id_type=MESH,
                    ).start()

                if (dy, dx, hz, hc) == (0, 0, 0, 0):
                    pl.when(parity != low)(start)
                else:
                    start()
    answer[mine] = back[0, 28]

    whole = answer.at[pl.ds(0, total - 1)]
    pltpu.make_async_copy(answer.at[pl.ds(0, 64)], answer.at[pl.ds(0, 64)], ds.at[1]).wait()
    pltpu.make_async_copy(whole, whole, br).wait()
    step = 512
    for j in range(model // step):
        here = slice(j * step, (j + 1) * step)
        answers = answer[:, :, here].astype(F32).reshape(4 * total, step).astype(BF)
        mixed = residual[:, here]
        for k in range(2):
            picked = lax.dot_general(
                onehot[k], answers, (((0,), (0,)), ((), ())), preferred_element_type=F32
            )
            mixed = mixed + picked * jnp.concatenate([gate[k]] * (step // tok), axis=1)
        out_ref[:, here] = mixed.astype(BF)
    pltpu.make_async_copy(whole, whole, bs).wait()


def body(
    queries, states, behavior_keys, behavior_values, lengths, user_of, out_weight, norm_gain,
    routes, route_weights, expert_up, expert_down,
):
    tok, model = queries.shape
    hist = behavior_keys.shape[1]
    ff = expert_up.shape[2]
    width = model // HEADS
    held = 8 * hist
    total = SEQS * GRPS
    hbm = pl.BlockSpec(memory_space=pltpu.HBM)
    vmem = pltpu.VMEM
    dma = pltpu.SemaphoreType.DMA
    return pl.pallas_call(
        block_kernel,
        out_shape=jax.ShapeDtypeStruct((tok, model), BF),
        in_specs=[hbm] * 12,
        out_specs=pl.BlockSpec(memory_space=vmem),
        scratch_shapes=[
            vmem((1, 2), jnp.int32),
            vmem((1, SEQS * tok), jnp.int32),
            vmem((2, tok), jnp.int32),
            vmem((tok, model), BF),
            vmem((2, hist, model), BF),
            vmem((2, hist, model), BF),
            vmem((SEQS, tok, width), BF),
            vmem((held, 2 * width), BF),
            vmem((held, 2 * width), BF),
            vmem((2 * width, SEQS * tok), BF),
            vmem((2 * width, held), BF),
            vmem((held, 4 * tok), F32),
            vmem((held, SEQS * tok), BF),
            vmem((2 * width, SEQS * tok), F32),
            vmem((SEQS, width, tok), BF),
            vmem((SEQS, width, tok), BF),
            vmem((SEQS, 8, tok), F32),
            vmem((SEQS, 8, tok), F32),
            vmem((2, tok), jnp.int32),
            vmem((2, tok), F32),
            vmem((tok, model), BF),
            vmem((1, model), F32),
            vmem((model, model), BF),
            vmem((model, ff), BF),
            vmem((ff, model), BF),
            vmem((2, 4 * total, tok), BF),
            vmem((2, tok, tok), F32),
            vmem((model, tok), BF),
            vmem((tok, model), F32),
            vmem((total, 4, model), BF),
            vmem((2, 2, total // 4, 4, model), BF),
            vmem((total, ff), BF),
            vmem((2, total // 4, 4, model), BF),
            vmem((total, 4, model), BF),
            dma((12,)),
            dma((5,)),
            dma, dma, dma, dma,
            dma((2,)),
            dma((2,)),
            dma, dma, dma, dma, dma, dma,
        ]
        + [dma((2,)), dma((2,)), dma, dma]
        + [pltpu.SemaphoreType.REGULAR],
        compiler_params=pltpu.CompilerParams(
            collective_id=0, has_side_effects=True, vmem_limit_bytes=VMEM_ALL
        ),
        name="decoder_block",
    )(
        queries, behavior_keys, behavior_values, lengths.reshape(1, -1), user_of.reshape(1, -1),
        routes.T, route_weights.T, states, norm_gain.reshape(1, -1), out_weight, expert_up,
        expert_down,
    )


def solution(mesh):
    return jax.shard_map(
        body,
        mesh=mesh,
        in_specs=(
            P(("grp", "seq"), None),
            P(("grp", "seq"), None),
            P("grp", "seq", None),
            P("grp", "seq", None),
            P("grp"),
            P("grp"),
            P(),
            P(),
            P(("grp", "seq"), None),
            P(("grp", "seq"), None),
            P(("seq", "grp"), None, None),
            P(("seq", "grp"), None, None),
        ),
        out_specs=P(("grp", "seq"), None),
        check_vma=False,
    )
```

```python
import itertools
import math

import jax
import jax.numpy as jnp
from jax import lax
from jax.experimental import pallas as pl
from jax.experimental.pallas import tpu as pltpu
from jax.sharding import PartitionSpec as P

HEADS = 8
MESH = pl.DeviceIdType.MESH
BF = jnp.bfloat16
F32 = jnp.float32
LOW = -1e30
VMEM_ALL = 67043328
SEQS = 16
GRPS = 8

FULL = ((0, 1), (0, 3), (1, 0), (3, 0))
FIRST = ((1, 1), (1, 3), (2, 0))
SECOND = ((3, 3), (3, 1), (0, 2))
HALVES = FIRST + SECOND

GROUPS = (
    ((2, 2), (2, 0), (0, 2), (0, 0)),
    ((2, 1), (1, 2), (2, 3), (3, 2), (0, 1), (1, 0), (0, 3), (3, 0)),
    ((1, 1), (3, 3), (1, 3), (3, 1)),
)


def head_of(y, z):
    return (y % 2) * 4 + (z + 2 * (y // 2)) % 4


def seq_of(y, z):
    return ((y + 8) % 4) * 4 + (z + 8) % 4


def far_first(steps):
    def hops(step):
        return sum(min(d, 4 - d) for d in step[:3])

    return sorted((s for s in steps if any(s)), key=lambda s: (-hops(s), sum(s) % 3, s))


def cols(head, width=128):
    return pl.ds(pl.multiple_of(head * width, width), width)


def block_kernel(
    q_hbm, k_hbm, v_hbm, len_hbm, user_hbm, routes_hbm, gates_hbm, states_hbm, gain_hbm,
    wo_hbm, up_hbm, down_hbm,
    out_ref,
    len_ref, user_ref, routes_ref, q_v, k_v, v_v, qbuf, kcat, vcat, qt, vt, score, prob, acc,
    osend, obuf, ssend, sbuf, rbuf,
    gates_ref, states_ref, gain_ref, wo, up, down,
    onehot, gate, att, residual, send, recv, hidden, back, answer,
    load_sem, own_sem, qs, qr, ks, kr, vs, vr, os, orr, ss, sr, rs, rr, ds, dr, bs, br, ready,
):
    me, g = lax.axis_index("seq"), lax.axis_index("grp")
    y, z = me // 4, me % 4
    head = head_of(y, z)
    hist = k_hbm.shape[1]
    half = hist // 2
    tok, model = q_hbm.shape
    ff = up.shape[1]
    width = model // HEADS
    scale = math.log2(math.e) / math.sqrt(width)
    total = SEQS * GRPS
    mine = me * GRPS + g
    parity = me % 2

    def load(i, src, dst):
        return pltpu.make_async_copy(src, dst, load_sem.at[i])

    loads = [
        load(0, q_hbm, q_v), load(1, k_hbm, k_v), load(2, v_hbm, v_v),
        load(3, routes_hbm, routes_ref), load(4, user_hbm, user_ref), load(5, len_hbm, len_ref),
        load(6, wo_hbm, wo), load(7, states_hbm, states_ref), load(8, gain_hbm, gain_ref),
        load(9, gates_hbm, gates_ref), load(10, up_hbm.at[0], up), load(11, down_hbm.at[0], down),
    ]
    for copy in loads[:6]:
        copy.start()
    own = [pltpu.make_async_copy(q_hbm.at[:, cols(head)], qbuf.at[me], own_sem.at[0])]
    for i, (src, dst) in enumerate(((k_hbm, kcat), (v_hbm, vcat))):
        for user in range(2):
            own.append(
                pltpu.make_async_copy(
                    src.at[user, :, cols(head)],
                    dst.at[pl.ds(0, hist), pl.ds(user * width, width)],
                    own_sem.at[1 + 2 * i + user],
                )
            )
    for copy in own:
        copy.start()

    barrier = pltpu.get_barrier_semaphore()
    seq_peers = [
        seq_of(y + dy, z + dz) for dy, dz in far_first(itertools.product(range(4), range(4)))
    ]
    for other in seq_peers:
        pl.semaphore_signal(barrier, inc=1, device_id={"seq": other}, device_id_type=MESH)
    for step in range(1, GRPS):
        pl.semaphore_signal(
            barrier, inc=1, device_id={"grp": (g + step) % GRPS}, device_id_type=MESH
        )
    pl.semaphore_wait(barrier, SEQS - 1 + GRPS - 1)

    partner = me + 1 - 2 * parity
    loads[3].wait()
    route_copy = pltpu.make_async_remote_copy(
        src_ref=routes_ref, dst_ref=rbuf, send_sem=rs, recv_sem=rr,
        device_id={"seq": partner}, device_id_type=MESH,
    )
    route_copy.start()
    loads[0].wait()
    for dy, dz in far_first(itertools.product(range(4), range(4))):
        ty, tz = (y + dy) % 4, (z + dz) % 4
        pltpu.make_async_remote_copy(
            src_ref=q_v.at[:, cols(head_of(ty, tz))],
            dst_ref=qbuf.at[me],
            send_sem=qs, recv_sem=qr,
            device_id={"seq": ty * 4 + tz}, device_id_type=MESH,
        ).start()

    def send_halves(src, dst, send_sem, recv_sem):
        for j, (dy, dz) in enumerate(HALVES):
            ty, tz = (y - dy + 4) % 4, (z - dz + 4) % 4
            first = 0 if (dy, dz) in FIRST else half
            for user in range(2):
                pltpu.make_async_remote_copy(
                    src_ref=src.at[user, pl.ds(first, half), cols(head_of(ty, tz))],
                    dst_ref=dst.at[pl.ds(5 * hist + j * half, half), pl.ds(user * width, width)],
                    send_sem=send_sem, recv_sem=recv_sem,
                    device_id={"seq": ty * 4 + tz}, device_id_type=MESH,
                ).start()

    def send_fulls(src, dst, send_sem, recv_sem):
        for j, (dy, dz) in enumerate(FULL):
            ty, tz = (y - dy + 4) % 4, (z - dz + 4) % 4
            for user in range(2):
                pltpu.make_async_remote_copy(
                    src_ref=src.at[user, :, cols(head_of(ty, tz))],
                    dst_ref=dst.at[pl.ds((1 + j) * hist, hist), pl.ds(user * width, width)],
                    send_sem=send_sem, recv_sem=recv_sem,
                    device_id={"seq": ty * 4 + tz}, device_id_type=MESH,
                ).start()

    loads[1].wait()
    send_halves(k_v, kcat, ks, kr)
    send_fulls(k_v, kcat, ks, kr)
    loads[2].wait()
    send_halves(v_v, vcat, vs.at[0], vr.at[0])
    send_fulls(v_v, vcat, vs.at[1], vr.at[1])

    for other in seq_peers:
        pl.semaphore_signal(ready, inc=1, device_id={"seq": other}, device_id_type=MESH)
    for copy in loads[6:]:
        copy.start()

    starts = []
    for dy, dz in ((0, 0),) + FULL:
        base = seq_of(y + dy, z + dz) * hist
        starts += [base, base + half]
    for dy, dz in HALVES:
        base = seq_of(y + dy, z + dz) * hist
        starts.append(base if (dy, dz) in FIRST else base + half)

    loads[4].wait()
    loads[5].wait()
    own[0].wait()
    moved = pl.ds(0, SEQS - 1)
    pltpu.make_async_copy(qbuf.at[moved], qbuf.at[moved], qr).wait()
    for i in range(SEQS):
        flipped = qbuf[i].T
        users = user_ref[:, i * tok : (i + 1) * tok]
        for user in range(2):
            qt[user * width : (user + 1) * width, i * tok : (i + 1) * tok] = jnp.where(
                users == user, flipped, jnp.zeros_like(flipped)
            )

    route_copy.wait()
    experts = lax.broadcasted_iota(jnp.int32, (total, tok), 0)
    named = [(routes_ref[k : k + 1, :] == experts).astype(F32) for k in range(2)]
    theirs = sum((rbuf[k : k + 1, :] == experts).astype(F32) for k in range(2))
    earlier = (
        lax.broadcasted_iota(jnp.int32, (tok, tok), 0) < lax.broadcasted_iota(jnp.int32, (tok, tok), 1)
    ).astype(BF)
    rank = jnp.dot((named[0] + named[1]).astype(BF), earlier, preferred_element_type=F32)
    ahead = jnp.dot(theirs.astype(BF), jnp.ones((tok, tok), BF), preferred_element_type=F32)
    rank = rank + ahead * parity.astype(F32)
    places = lax.broadcasted_iota(jnp.int32, (4 * total, tok), 0)
    loads[9].wait()
    for k in range(2):
        slot = jnp.sum(named[k] * rank, axis=0, keepdims=True).astype(jnp.int32)
        target = routes_ref[k : k + 1, :] * 4 + slot
        onehot[k] = (places == target).astype(F32).astype(BF)
        gate[k] = jnp.broadcast_to(gates_ref[k : k + 1, :], (tok, tok)).T

    own[1].wait()
    own[2].wait()
    far = pl.ds(5 * hist, 6 * half)
    near = pl.ds(hist, 4 * hist)
    rest = pl.ds(hist, kcat.shape[0] - hist)
    pltpu.make_async_copy(kcat.at[rest], kcat.at[rest], kr).wait()

    block = 4 * tok
    rows_y = [(y + dy) % 4 for dy in (2, 1, 3, 0)]
    limit0 = len_ref[0:1, 0:1]
    limit1 = len_ref[0:1, 1:2]

    def tokens_of(row):
        return pl.ds(pl.multiple_of(row * block, block), block)

    stat = []
    for row in rows_y:
        here = tokens_of(row)
        limit = jnp.where(user_ref[:, here] == 0, limit0, limit1)
        top = jnp.full((8, block), LOW, F32)
        for c, start in enumerate(starts):
            s = jnp.dot(kcat[c * half : (c + 1) * half, :], qt[:, here], preferred_element_type=F32)
            pos = start + lax.broadcasted_iota(jnp.int32, (half, block), 0)
            s = jnp.where(pos < limit, s, LOW)
            score[c * half : (c + 1) * half, :] = s
            top = jnp.maximum(top, s.reshape(half // 8, 8, block).max(0))
        peak = top.max(0, keepdims=True)
        denom = jnp.zeros((8, block), F32)
        for c in range(len(starts)):
            p = jnp.exp2((score[c * half : (c + 1) * half, :] - peak) * scale)
            denom = denom + p.reshape(half // 8, 8, block).sum(0)
            prob[c * half : (c + 1) * half, here] = p.astype(BF)
        stat.append((peak, denom.sum(0, keepdims=True)))

    own[3].wait()
    own[4].wait()
    pltpu.make_async_copy(vcat.at[far], vcat.at[far], vr.at[0]).wait()
    split = 5 * hist
    vt[:, split:] = vcat[split:, :].T
    for row in rows_y:
        here = tokens_of(row)
        acc[:, here] = jnp.dot(vt[:, split:], prob[split:, here], preferred_element_type=F32)
    pltpu.make_async_copy(vcat.at[near], vcat.at[near], vr.at[1]).wait()
    vt[:, :split] = vcat[:split, :].T

    for row, (peak, denom) in zip(rows_y, stat):
        here = tokens_of(row)
        both = acc[:, here] + jnp.dot(vt[:, :split], prob[:split, here], preferred_element_type=F32)
        out = jnp.where(user_ref[:, here] == 0, both[:width], both[width:]) * (1.0 / denom)
        out = out.astype(BF)
        packed = jnp.concatenate([peak, denom], axis=0)
        for i in range(4):
            osend[row * 4 + i] = out[:, i * tok : (i + 1) * tok]
            ssend[row * 4 + i] = packed[:, i * tok : (i + 1) * tok]
        for dz in (2, 1, 3, 0):
            owner = row * 4 + (z + dz) % 4
            if dz == 0 and row is rows_y[-1]:
                continue
            pltpu.make_async_remote_copy(
                src_ref=osend.at[owner], dst_ref=obuf.at[me], send_sem=os, recv_sem=orr,
                device_id={"seq": owner}, device_id_type=MESH,
            ).start()
            pltpu.make_async_remote_copy(
                src_ref=ssend.at[owner], dst_ref=sbuf.at[me], send_sem=ss, recv_sem=sr,
                device_id={"seq": owner}, device_id_type=MESH,
            ).start()

    obuf[me] = osend[me]
    sbuf[me] = ssend[me]
    pltpu.make_async_copy(qbuf.at[moved], qbuf.at[moved], qs).wait()
    pltpu.make_async_copy(kcat.at[rest], kcat.at[rest], ks).wait()
    pltpu.make_async_copy(vcat.at[far], vcat.at[far], vs.at[0]).wait()
    pltpu.make_async_copy(vcat.at[near], vcat.at[near], vs.at[1]).wait()
    for i in (6, 7, 8):
        loads[i].wait()

    pl.semaphore_wait(ready, SEQS - 1)

    pltpu.make_async_copy(sbuf.at[moved], sbuf.at[moved], sr).wait()
    pltpu.make_async_copy(obuf.at[moved], obuf.at[moved], orr).wait()
    for h in range(HEADS):
        hy, hz = h // 4, h % 4
        first = hy * 4 + hz
        second = (hy + 2) * 4 + (hz + 2) % 4
        m0, d0 = sbuf[first, 0:1], sbuf[first, 1:2]
        m1, d1 = sbuf[second, 0:1], sbuf[second, 1:2]
        top = jnp.maximum(m0, m1)
        w0 = d0 * jnp.exp2((m0 - top) * scale)
        w1 = d1 * jnp.exp2((m1 - top) * scale)
        inverse = 1.0 / (w0 + w1)
        merged = obuf[first].astype(F32) * (w0 * inverse) + obuf[second].astype(F32) * (w1 * inverse)
        att[h * width : (h + 1) * width, :] = merged.astype(BF)

    res = states_ref[...].astype(F32) + lax.dot_general(
        att[...], wo[...], (((0,), (0,)), ((), ())), preferred_element_type=F32
    )
    residual[...] = res
    spread = jnp.mean(res * res, axis=-1, keepdims=True)
    normed = (res / jnp.sqrt(spread + 1e-06) * gain_ref[...]).astype(BF)
    placed = onehot[0] + onehot[1]

    zh, x, core = z // 2, g // 2, g % 2

    def peers(n, sign):
        before = sum(len(steps) for steps in GROUPS[:n])
        for k, (dy, dx) in enumerate(GROUPS[n]):
            for hz, hc, low in itertools.product(range(2), range(2), range(2)):
                other = (y + sign * dy + 4) % 4 * 4 + (zh + hz) % 2 * 2 + low
                og = (x + sign * dx + 4) % 4 * 2 + (core + hc) % 2
                here = (dy, dx, hz, hc) == (0, 0, 0, 0)
                yield (before + k) * 4 + hz * 2 + hc, other, og, low if here else None

    home = 4 * [step for steps in GROUPS for step in steps].index((0, 0))

    def remote(n):
        return answer.at[pl.ds(0, 8 * len(GROUPS[n]) - ((0, 0) in GROUPS[n]))]

    send[...] = (
        jnp.dot(placed, normed, preferred_element_type=F32).reshape(total, 4, model).astype(BF)
    )
    for n in range(len(GROUPS)):
        if n > 0:
            pltpu.make_async_copy(remote(n - 1), remote(n - 1), ds.at[n - 1]).wait()
        for slot, other, og, low in peers(n, -1):
            def start(slot=slot, other=other, og=og, n=n):
                pltpu.make_async_remote_copy(
                    src_ref=send.at[other * GRPS + og], dst_ref=recv.at[parity, slot],
                    send_sem=ds.at[n], recv_sem=dr.at[n],
                    device_id={"seq": other, "grp": og}, device_id_type=MESH,
                ).start()

            if low is None:
                start()
            else:
                pl.when(parity != low)(start)
    recv[parity, home] = send[mine]

    pltpu.make_async_copy(obuf.at[moved], obuf.at[moved], os).wait()
    pltpu.make_async_copy(sbuf.at[moved], sbuf.at[moved], ss).wait()
    loads[10].wait()
    loads[11].wait()
    for n, steps in enumerate(GROUPS):
        pltpu.make_async_copy(remote(n), remote(n), dr.at[n]).wait()
        low = 4 * sum(len(before) for before in GROUPS[:n])
        held = slice(low, low + 4 * len(steps))
        count = 16 * len(steps)
        rows = recv[0, held].astype(F32) + recv[1, held].astype(F32)
        rows = rows.reshape(count, model).astype(BF)
        step = 512
        for j in range(ff // step):
            here = slice(j * step, (j + 1) * step)
            hidden[:count, here] = jax.nn.gelu(
                jnp.dot(rows, up[:, here], preferred_element_type=F32)
            ).astype(BF)
        step = 256
        for j in range(model // step):
            here = slice(j * step, (j + 1) * step)
            back[held, :, here] = (
                jnp.dot(hidden[:count, :], down[:, here], preferred_element_type=F32)
                .reshape(4 * len(steps), 4, step)
                .astype(BF)
            )
        for slot, other, og, low in peers(n, 1):
            def start(slot=slot, other=other, og=og):
                pltpu.make_async_remote_copy(
                    src_ref=back.at[slot], dst_ref=answer.at[mine], send_sem=bs, recv_sem=br,
                    device_id={"seq": other, "grp": og}, device_id_type=MESH,
                ).start()

            if low is None:
                start()
            else:
                pl.when(parity != low)(start)
    answer[mine] = back[home]

    whole = answer.at[pl.ds(0, total - 1)]
    pltpu.make_async_copy(remote(len(GROUPS) - 1), remote(len(GROUPS) - 1), ds.at[len(GROUPS) - 1]).wait()
    pltpu.make_async_copy(whole, whole, br).wait()
    step = 512
    for j in range(model // step):
        here = slice(j * step, (j + 1) * step)
        answers = answer[:, :, here].astype(F32).reshape(4 * total, step).astype(BF)
        mixed = residual[:, here]
        for k in range(2):
            picked = lax.dot_general(
                onehot[k], answers, (((0,), (0,)), ((), ())), preferred_element_type=F32
            )
            mixed = mixed + picked * jnp.concatenate([gate[k]] * (step // tok), axis=1)
        out_ref[:, here] = mixed.astype(BF)
    pltpu.make_async_copy(whole, whole, bs).wait()


def body(
    queries, states, behavior_keys, behavior_values, lengths, user_of, out_weight, norm_gain,
    routes, route_weights, expert_up, expert_down,
):
    tok, model = queries.shape
    hist = behavior_keys.shape[1]
    ff = expert_up.shape[2]
    width = model // HEADS
    held = 8 * hist
    total = SEQS * GRPS
    hbm = pl.BlockSpec(memory_space=pltpu.HBM)
    vmem = pltpu.VMEM
    dma = pltpu.SemaphoreType.DMA
    return pl.pallas_call(
        block_kernel,
        out_shape=jax.ShapeDtypeStruct((tok, model), BF),
        in_specs=[hbm] * 12,
        out_specs=pl.BlockSpec(memory_space=vmem),
        scratch_shapes=[
            vmem((1, 2), jnp.int32),
            vmem((1, SEQS * tok), jnp.int32),
            vmem((2, tok), jnp.int32),
            vmem((tok, model), BF),
            vmem((2, hist, model), BF),
            vmem((2, hist, model), BF),
            vmem((SEQS, tok, width), BF),
            vmem((held, 2 * width), BF),
            vmem((held, 2 * width), BF),
            vmem((2 * width, SEQS * tok), BF),
            vmem((2 * width, held), BF),
            vmem((held, 4 * tok), F32),
            vmem((held, SEQS * tok), BF),
            vmem((2 * width, SEQS * tok), F32),
            vmem((SEQS, width, tok), BF),
            vmem((SEQS, width, tok), BF),
            vmem((SEQS, 2, tok), F32),
            vmem((SEQS, 2, tok), F32),
            vmem((2, tok), jnp.int32),
            vmem((2, tok), F32),
            vmem((tok, model), BF),
            vmem((1, model), F32),
            vmem((model, model), BF),
            vmem((model, ff), BF),
            vmem((ff, model), BF),
            vmem((2, 4 * total, tok), BF),
            vmem((2, tok, tok), F32),
            vmem((model, tok), BF),
            vmem((tok, model), F32),
            vmem((total, 4, model), BF),
            vmem((2, total // 2, 4, model), BF),
            vmem((16 * max(len(steps) for steps in GROUPS), ff), BF),
            vmem((total // 2, 4, model), BF),
            vmem((total, 4, model), BF),
            dma((12,)),
            dma((5,)),
            dma, dma, dma, dma,
            dma((2,)),
            dma((2,)),
            dma, dma, dma, dma, dma, dma,
        ]
        + [dma((len(GROUPS),)), dma((len(GROUPS),)), dma, dma]
        + [pltpu.SemaphoreType.REGULAR],
        compiler_params=pltpu.CompilerParams(
            collective_id=0, has_side_effects=True, vmem_limit_bytes=VMEM_ALL
        ),
        name="decoder_block",
    )(
        queries, behavior_keys, behavior_values, lengths.reshape(1, -1), user_of.reshape(1, -1),
        routes.T, route_weights.T, states, norm_gain.reshape(1, -1), out_weight, expert_up,
        expert_down,
    )


def solution(mesh):
    return jax.shard_map(
        body,
        mesh=mesh,
        in_specs=(
            P(("grp", "seq"), None),
            P(("grp", "seq"), None),
            P("grp", "seq", None),
            P("grp", "seq", None),
            P("grp"),
            P("grp"),
            P(),
            P(),
            P(("grp", "seq"), None),
            P(("grp", "seq"), None),
            P(("seq", "grp"), None, None),
            P(("seq", "grp"), None, None),
        ),
        out_specs=P(("grp", "seq"), None),
        check_vma=False,
    )
```
